128 devices in a mesh: row: 16 (over z, y_hi, core), col: 8 (over y_lo, x).
Axes of the slice: x: 4, y: 4 (y_hi: 2, y_lo: 2; y = y_hi * 2 + y_lo), z: 4, core: 2. Of those that a mesh axis runs over, the one named last changes fastest.
Arguments:
- velocity: float32 [3, 128, 128, 128], P(None, 'row', 'col'), may hold values from -6 to 6
Outputs:
- advanced: float32 [3, 128, 128, 128], P(None, 'row', 'col')
The draws below stay inside these ranges and needn't reach their ends.
All inputs are finite; a program needn't handle non-finite values.
Results may differ from the reference program's by a relative error of at most 0.0003.
Values sent between devices are 32-bit elements.
No kernel may reach another device: no remote copies, remote signals or barrier semaphores. Data moves between devices by JAX's collectives and lax.ppermute only.
A program may use at most 64 MiB of HBM per device.

```python
import jax
import jax.numpy as jnp

N = 128


def block_levels(key, shape, pieces, least, top_value):
    loudness = 1.0
    for axis_at, shards_of in pieces:
        draws = jax.random.uniform(jax.random.fold_in(jax.random.fold_in(key, 6), axis_at), (shards_of,), jnp.float32, least / len(pieces), top_value / len(pieces))
        loudness = loudness * jnp.repeat(jnp.exp(draws), shape[axis_at] // shards_of).reshape((-1,) + (1,) * (len(shape) - 1 - axis_at))
    return loudness


def scatter_about(key, extent, deviation, bound, shards=(), held_as=jnp.bfloat16):
    loudness = block_levels(key, extent, shards, -0.22, 0.18) if shards else 1.0
    array = jax.random.normal(key, extent, jnp.float32) * deviation * loudness
    return jnp.minimum(jnp.maximum(array, -bound), bound).astype(held_as)


def setup_inputs(seed: int = 0) -> dict:
    arg_keys = jax.random.split(jax.random.key(seed), 2)
    return {
        "velocity": scatter_about(arg_keys[0], (3, N, N, N), 1.0, 6.0, ((1, 16), (2, 8)), jnp.float32),
    }


def spectrum(field):
    return jnp.fft.rfftn(field, axes=(1, 2, 3), norm="forward")[..., : N // 2]


def grid_field(spectral):
    nyquist = jnp.zeros(spectral.shape[:3] + (1,), spectral.dtype)
    padded = jnp.concatenate([spectral, nyquist], axis=3)
    return jnp.fft.irfftn(padded, s=(N, N, N), axes=(1, 2, 3), norm="forward")


def wave_numbers():
    index = jnp.arange(N, dtype=jnp.int32)
    signed = jnp.where(index < N // 2, index, index - N)
    half = jnp.arange(N // 2, dtype=jnp.int32)
    return signed[:, None, None], signed[None, :, None], half[None, None, :]


def cross_with(left, right):
    return jnp.stack([left[1] * right[2] - left[2] * right[1], left[2] * right[0] - left[0] * right[2], left[0] * right[1] - left[1] * right[0]])


def reference(velocity):
    int_waves = wave_numbers()
    mask = ((3 * jnp.abs(int_waves[0]) < N) & (3 * jnp.abs(int_waves[1]) < N) & (3 * jnp.abs(int_waves[2]) < N)).astype(jnp.float32)
    waves = [wave.astype(jnp.float32) for wave in int_waves]
    squared = waves[0] * waves[0] + waves[1] * waves[1] + waves[2] * waves[2]
    safe_norm = jnp.where(squared > 0, squared, jnp.float32(1.0))
    viscous = squared / N
    step = 2.0 / N

    def project(field):
        along = (waves[0] * field[0] + waves[1] * field[1] + waves[2] * field[2]) / safe_norm
        return field - jnp.stack([waves[0] * along, waves[1] * along, waves[2] * along])

    def tendency(state):
        flow = grid_field(state)
        spin = grid_field(1j * cross_with(waves, state))
        product = cross_with(flow, spin)
        return project(mask * spectrum(product)) - viscous * state

    start = project(mask * spectrum(velocity))
    first = tendency(start)
    second = tendency(start + step * first)
    return grid_field(start + 0.5 * step * (first + second)).astype(jnp.float32)
```

```python
import jax
import jax.numpy as jnp
import ml_dtypes
import numpy as np
from jax import lax
from jax.experimental import pallas as pl
from jax.experimental.pallas import tpu as pltpu
from jax.sharding import PartitionSpec as P

N = 128
KX = 96
SLOTS = 32
f32, bf16 = jnp.float32, jnp.bfloat16


def owners():
    kz = np.array([1 + d // 3 for d in range(126)] + [0, 0])
    third = np.array([d % 3 for d in range(126)] + [0, 1])
    ky = np.zeros((4, SLOTS), np.int64)
    ok = np.zeros((4, SLOTS), bool)
    ky[0], ok[0] = np.arange(32), True
    ky[1], ok[1] = np.concatenate([np.arange(32, 43), np.arange(-42, -21)]), True
    ky[2, :21], ok[2, :21] = np.arange(-21, 0), True
    return kz, third, ky, ok


def split(a):
    hi = a.astype(np.float32).astype(ml_dtypes.bfloat16)
    lo = (a - hi.astype(np.float64)).astype(np.float32).astype(ml_dtypes.bfloat16)
    return hi, lo


def left(a, pad=0):
    hi, lo = split(a)
    zero = np.zeros((a.shape[0], pad), hi.dtype)
    return np.concatenate([hi, hi, lo, zero], axis=1)


def right(a):
    hi, lo = split(a)
    return np.concatenate([hi, hi, lo], axis=0)


def tables():
    kz, third, ky, ok = owners()
    cell = np.arange(N)

    def angle(a, b):
        return 2 * np.pi * (np.multiply.outer(a, b) % N) / N

    az = angle(kz, cell)
    z_fwd = left(np.concatenate([np.cos(az), -np.sin(az)], axis=0))
    z_inv = left(np.concatenate([np.cos(az.T), -np.sin(az.T)], axis=1))
    ay = angle(ky.reshape(-1), cell)
    keep = ok.reshape(-1)[:, None]
    cy, sy = np.cos(ay) * keep, np.sin(ay) * keep
    y_inv = right(np.block([[cy, sy], [-sy, cy]]))
    y_fwd = right(np.block([[cy.T, -sy.T], [sy.T, cy.T]]))
    ax = angle(np.arange(KX) - 42, cell)
    keep = (np.arange(KX) < 85)[:, None]
    cx, sx = np.cos(ax) * keep, np.sin(ax) * keep
    x_fwd = left(np.block([[cx, sx], [-sx, cx]]))
    x_inv = left(np.block([[cx.T, -sx.T], [sx.T, cx.T]]), 64)
    mask = (np.repeat(np.arange(4), SLOTS)[None, :] == third[:, None]).astype(np.float32)
    lanes = np.zeros((N, 16, N), np.float32)
    group, slot = np.repeat(np.arange(4), SLOTS), np.tile(np.arange(SLOTS), 4)
    for d in range(N):
        c = (group - third[d]) % 4
        y = ky[third[d]][slot].astype(np.float64)
        z = float(kz[d])
        good = ok[third[d]][slot] & (c < 3) & ((kz[d] > 0) | (y >= 0))
        count = np.where((kz[d] == 0) & (y == 0), 1.0, 2.0)

        def component(which):
            return (which == 0) * (c < 3), ((which == 1) * y + (which == 2) * z) * (c < 3)

        lanes[d, 0], lanes[d, 1] = component(c)
        lanes[d, 2], lanes[d, 3] = component((c + 1) % 3)
        lanes[d, 4], lanes[d, 5] = component((c + 2) % 3)
        lanes[d, 6] = y * y + z * z
        lanes[d, 7] = good * count / float(N) ** 3
        lanes[d, 8], lanes[d, 9] = c == 2, c == 0
        lanes[d, 10] = group == third[d]
    return dict(z_fwd=z_fwd, z_inv=z_inv, y_fwd=y_fwd, y_inv=y_inv, x_fwd=x_fwd, x_inv=x_inv, mask=mask, lanes=lanes)


def halves(a):
    hi = a.astype(bf16)
    return hi, (a - hi.astype(f32)).astype(bf16)


def dot(a, b):
    return jnp.dot(a, b, preferred_element_type=f32)


def apply_left(table, rows, pad=0):
    hi, lo = halves(rows)
    stack = [hi, lo, hi]
    if pad:
        stack.append(jnp.zeros((pad, rows.shape[1]), bf16))
    return dot(table, jnp.concatenate(stack, axis=0))


def apply_right(columns, table):
    hi, lo = halves(columns)
    return dot(jnp.concatenate([hi, lo, hi], axis=1), table)


def turn(a, groups):
    shift = (groups * SLOTS) % N
    return pltpu.roll(a, shift, 1) if shift else a


def swap_blocks(a):
    a = a.reshape(16, 8, N)
    row = lax.broadcasted_iota(jnp.int32, a.shape, 1)
    block = lax.broadcasted_iota(jnp.int32, a.shape, 2) // 16
    for bit in (4, 2, 1):
        same = (row & bit) == (block & bit)
        up = pltpu.roll(pltpu.roll(a, 16 * bit, 2), 8 - bit, 1)
        if bit == 4:
            a = jnp.where(same, a, up)
        else:
            down = pltpu.roll(pltpu.roll(a, N - 16 * bit, 2), bit, 1)
            a = jnp.where(same, a, jnp.where((row & bit) == 0, up, down))
    return a.reshape(N, N)


def every(ref, j, count):
    return ref[pl.ds(j, N, count), :]


def pencil_to_rows(v, z_fwd, out):
    turned = jnp.concatenate([v[c * N : (c + 1) * N, :].T for c in range(3)], axis=1)
    waves = apply_left(z_fwd[...], turned)
    for part in range(2):
        for c in range(3):
            out[pl.ds(part * 3 + c, N, 6), :] = waves[part * N : (part + 1) * N, c * N : (c + 1) * N]


def rows_to_pencil(rows, z_inv, out):
    stack = jnp.concatenate(
        [jnp.concatenate([every(rows, part * 3 + c, 6) for c in range(3)], axis=1) for part in range(2)], axis=0
    )
    cells = apply_left(z_inv[...], stack)
    for c in range(3):
        out[c * N : (c + 1) * N, :] = cells[:, c * N : (c + 1) * N].T


def y_forward(pairs, mask, table):
    spectrum = apply_right(jnp.concatenate([jnp.concatenate(p, axis=1) for p in pairs], axis=0), table)
    real, imaginary = 0.0, 0.0
    for c in range(3):
        block = spectrum[c * N : (c + 1) * N]
        real = real + turn(block[:, :N] * mask, c)
        imaginary = imaginary + turn(block[:, N:] * mask, c)
    return real, imaginary


def y_inverse(pairs, mask, table):
    stack = [
        jnp.concatenate([turn(part, -c) * mask for part in pair], axis=1) for pair in pairs for c in range(3)
    ]
    return apply_right(jnp.concatenate(stack, axis=0), table)


def slab(rows, mask, z_fwd, z_inv, y_fwd, y_inv, out):
    mask = mask[...]
    pairs = [(every(rows, 2 * j, 4), every(rows, 2 * j + 1, 4)) for j in range(2)]
    lines = y_inverse(pairs, mask, y_inv[...])
    fields = [lines[f * N : (f + 1) * N] for f in range(6)]
    stack = jnp.concatenate(
        [jnp.concatenate([a[:, part * N : (part + 1) * N] for a in fields], axis=1) for part in range(2)], axis=0
    )
    grid = apply_left(z_inv[...], stack)
    u = [grid[:, c * N : (c + 1) * N] for c in range(3)]
    w = [grid[:, (3 + c) * N : (4 + c) * N] for c in range(3)]
    product = jnp.concatenate(
        [u[1] * w[2] - u[2] * w[1], u[2] * w[0] - u[0] * w[2], u[0] * w[1] - u[1] * w[0]], axis=1
    )
    waves = apply_left(z_fwd[...], product)
    pairs = [(waves[:N, c * N : (c + 1) * N], waves[N:, c * N : (c + 1) * N]) for c in range(3)]
    real, imaginary = y_forward(pairs, mask, y_fwd[...])
    out[pl.ds(0, N, 2), :] = real
    out[pl.ds(1, N, 2), :] = imaginary


class Waves:
    def __init__(self, lanes):
        kx = (lax.broadcasted_iota(jnp.int32, (KX, N), 0) - 42).astype(f32)

        def lane(i):
            return lanes[i : i + 1, :]

        self.own = kx * lane(0) + lane(1)
        self.after = kx * lane(2) + lane(3)
        self.before = kx * lane(4) + lane(5)
        self.squared = kx * kx + lane(6)
        self.inverse = 1.0 / jnp.where(self.squared > 0, self.squared, 1.0)
        self.scale = lane(7)
        self.is_last = jnp.broadcast_to(lane(8), (KX, N)) > 0
        self.is_first = jnp.broadcast_to(lane(9), (KX, N)) > 0
        self.third = lane(10)

    def project(self, part):
        part = part * self.scale
        along = part * self.own
        along = along + turn(along, 1)
        along = along + turn(along, 2)
        return part - self.own * (along * self.inverse)

    def cross(self, part):
        two = turn(part, 2)
        after = jnp.where(self.is_last, two, turn(part, -1))
        before = jnp.where(self.is_first, two, turn(part, 1))
        return self.after * before - self.before * after


def x_forward(real, imaginary, table):
    waves = apply_left(table, jnp.concatenate([real, imaginary], axis=0))
    return waves[:KX], waves[KX:]


def send_fields(waves, state, x_inv, out):
    curl = (-waves.cross(state[1]), waves.cross(state[0]))
    stack = jnp.concatenate([jnp.concatenate([state[i], curl[i]], axis=1) for i in range(2)], axis=0)
    lines = apply_left(x_inv[...], stack, 64)
    for field in range(2):
        for part in range(2):
            out[pl.ds(2 * field + part, N, 4), :] = lines[part * N : (part + 1) * N, field * N : (field + 1) * N]


def start_modes(rows, lanes, y_fwd, x_fwd, x_inv, out, state_out):
    waves = Waves(lanes)
    planes = [swap_blocks(every(rows, j, 6)) for j in range(6)]
    real, imaginary = y_forward([(planes[c], planes[3 + c]) for c in range(3)], waves.third, y_fwd[...])
    state = [waves.project(part) for part in x_forward(real, imaginary, x_fwd[...])]
    for i in range(2):
        state_out[i * KX : (i + 1) * KX, :] = state[i]
    send_fields(waves, state, x_inv, out)


def tendency(waves, rows, x_fwd, state):
    parts = x_forward(every(rows, 0, 2), every(rows, 1, 2), x_fwd[...])
    viscous = waves.squared * (1.0 / N)
    return [waves.project(parts[i]) - viscous * state[i] for i in range(2)]


def middle_modes(rows, lanes, x_fwd, x_inv, state_in, out, middle_out, half_out):
    waves = Waves(lanes)
    state = [state_in[i * KX : (i + 1) * KX, :] for i in range(2)]
    first = tendency(waves, rows, x_fwd, state)
    step = 2.0 / N
    middle = [state[i] + step * first[i] for i in range(2)]
    for i in range(2):
        middle_out[i * KX : (i + 1) * KX, :] = middle[i]
        half_out[i * KX : (i + 1) * KX, :] = state[i] + 0.5 * step * first[i]
    send_fields(waves, middle, x_inv, out)


def final_modes(rows, lanes, x_fwd, x_inv, y_inv, middle_in, half_in, out):
    waves = Waves(lanes)
    middle = [middle_in[i * KX : (i + 1) * KX, :] for i in range(2)]
    second = tendency(waves, rows, x_fwd, middle)
    final = [half_in[i * KX : (i + 1) * KX, :] + (1.0 / N) * second[i] for i in range(2)]
    lines = apply_left(x_inv[...], jnp.concatenate(final, axis=0), 64)
    cells = y_inverse([(lines[:N], lines[N:])], waves.third, y_inv[...])
    for c in range(3):
        for part in range(2):
            plane = cells[c * N : (c + 1) * N, part * N : (part + 1) * N]
            out[pl.ds(part * 3 + c, N, 6), :] = swap_blocks(plane)


def call(kernel, outs):
    shapes = [jax.ShapeDtypeStruct(s, f32) for s in outs]
    return pl.pallas_call(kernel, out_shape=shapes if len(shapes) > 1 else shapes[0], name=kernel.__name__)


def exchange(rows):
    count = rows.shape[0] // N
    rows = rows.reshape(N, 1, count * N)
    rows = lax.all_to_all(rows, ("row", "col"), split_axis=0, concat_axis=0, tiled=True)
    return rows.reshape(N * count, N)


TABLES = tables()


def local(velocity):
    t = {name: jnp.asarray(value) for name, value in TABLES.items()}
    device = lax.axis_index("row") * lax.axis_size("col") + lax.axis_index("col")
    lanes = lax.dynamic_index_in_dim(t["lanes"], device, 0, keepdims=False)
    kept = (2 * KX, N)

    def physical(rows):
        return call(slab, [(2 * N, N)])(rows, t["mask"], t["z_fwd"], t["z_inv"], t["y_fwd"], t["y_inv"])

    shape = velocity.shape
    rows = exchange(call(pencil_to_rows, [(6 * N, N)])(velocity.reshape(3 * N, N), t["z_fwd"]))
    rows, state = call(start_modes, [(4 * N, N), kept])(rows, lanes, t["y_fwd"], t["x_fwd"], t["x_inv"])
    rows = exchange(physical(exchange(rows)))
    rows, middle, half = call(middle_modes, [(4 * N, N), kept, kept])(rows, lanes, t["x_fwd"], t["x_inv"], state)
    rows = exchange(physical(exchange(rows)))
    rows = call(final_modes, [(6 * N, N)])(rows, lanes, t["x_fwd"], t["x_inv"], t["y_inv"], middle, half)
    return call(rows_to_pencil, [(3 * N, N)])(exchange(rows), t["z_inv"]).reshape(shape)


def solution(mesh):
    placed = P(None, "row", "col", None)
    return jax.shard_map(local, mesh=mesh, in_specs=(placed,), out_specs=placed, check_vma=False)
```

```python
import jax
import jax.numpy as jnp
import ml_dtypes
import numpy as np
from jax import lax
from jax.experimental import pallas as pl
from jax.experimental.pallas import tpu as pltpu
from jax.sharding import PartitionSpec as P

N = 128
KX = 96
SLOTS = 32
f32, bf16 = jnp.float32, jnp.bfloat16


def owners():
    kz = np.array([1 + d // 3 for d in range(126)] + [0, 0])
    third = np.array([d % 3 for d in range(126)] + [0, 1])
    ky = np.zeros((4, SLOTS), np.int64)
    ok = np.zeros((4, SLOTS), bool)
    ky[0], ok[0] = np.arange(32), True
    ky[1], ok[1] = np.concatenate([np.arange(32, 43), np.arange(-42, -21)]), True
    ky[2, :21], ok[2, :21] = np.arange(-21, 0), True
    return kz, third, ky, ok


def split(a):
    hi = a.astype(np.float32).astype(ml_dtypes.bfloat16)
    lo = (a - hi.astype(np.float64)).astype(np.float32).astype(ml_dtypes.bfloat16)
    return hi, lo


def left(a, pad=0):
    hi, lo = split(a)
    zero = np.zeros((a.shape[0], pad), hi.dtype)
    return np.concatenate([hi, hi, lo, zero], axis=1)


def right(a):
    hi, lo = split(a)
    return np.concatenate([hi, hi, lo], axis=0)


def tables():
    kz, third, ky, ok = owners()
    cell = np.arange(N)

    def angle(a, b):
        return 2 * np.pi * (np.multiply.outer(a, b) % N) / N

    az = angle(kz, cell)
    z_fwd = left(np.concatenate([np.cos(az), -np.sin(az)], axis=0))
    z_inv = left(np.concatenate([np.cos(az.T), -np.sin(az.T)], axis=1))
    ay = angle(ky.reshape(-1), cell)
    keep = ok.reshape(-1)[:, None]
    cy, sy = np.cos(ay) * keep, np.sin(ay) * keep
    y_inv = right(np.block([[cy, sy], [-sy, cy]]))
    y_fwd = right(np.block([[cy.T, -sy.T], [sy.T, cy.T]]))
    ax = angle(np.arange(KX) - 42, cell)
    keep = (np.arange(KX) < 85)[:, None]
    cx, sx = np.cos(ax) * keep, np.sin(ax) * keep
    x_fwd = left(np.block([[cx, sx], [-sx, cx]]))
    x_inv = left(np.block([[cx.T, -sx.T], [sx.T, cx.T]]), 64)
    mask = (np.repeat(np.arange(4), SLOTS)[None, :] == third[:, None]).astype(np.float32)
    lanes = np.zeros((N, 16, N), np.float32)
    group, slot = np.repeat(np.arange(4), SLOTS), np.tile(np.arange(SLOTS), 4)
    for d in range(N):
        c = (group - third[d]) % 4
        y = ky[third[d]][slot].astype(np.float64)
        z = float(kz[d])
        good = ok[third[d]][slot] & (c < 3) & ((kz[d] > 0) | (y >= 0))
        count = np.where((kz[d] == 0) & (y == 0), 1.0, 2.0)

        def component(which):
            return (which == 0) * (c < 3), ((which == 1) * y + (which == 2) * z) * (c < 3)

        lanes[d, 0], lanes[d, 1] = component(c)
        lanes[d, 2], lanes[d, 3] = component((c + 1) % 3)
        lanes[d, 4], lanes[d, 5] = component((c + 2) % 3)
        lanes[d, 6] = y * y + z * z
        lanes[d, 7] = good * count / float(N) ** 3
        lanes[d, 8], lanes[d, 9] = c == 2, c == 0
        lanes[d, 10] = group == third[d]
    return dict(z_fwd=z_fwd, z_inv=z_inv, y_fwd=y_fwd, y_inv=y_inv, x_fwd=x_fwd, x_inv=x_inv, mask=mask, lanes=lanes)


def halves(a):
    hi = a.astype(bf16)
    return hi, (a - hi.astype(f32)).astype(bf16)


def dot(a, b):
    return jnp.dot(a, b, preferred_element_type=f32)


def apply_left(table, rows, pad=0):
    hi, lo = halves(rows)
    stack = [hi, lo, hi]
    if pad:
        stack.append(jnp.zeros((pad, rows.shape[1]), bf16))
    return dot(table, jnp.concatenate(stack, axis=0))


def apply_right(columns, table):
    hi, lo = halves(columns)
    return dot(jnp.concatenate([hi, lo, hi], axis=1), table)


def turn(a, groups):
    shift = (groups * SLOTS) % N
    return pltpu.roll(a, shift, 1) if shift else a


def swap_blocks(a):
    a = a.reshape(16, 8, N)
    row = lax.broadcasted_iota(jnp.int32, a.shape, 1)
    block = lax.broadcasted_iota(jnp.int32, a.shape, 2) // 16
    for bit in (4, 2, 1):
        same = (row & bit) == (block & bit)
        up = pltpu.roll(pltpu.roll(a, 16 * bit, 2), 8 - bit, 1)
        if bit == 4:
            a = jnp.where(same, a, up)
        else:
            down = pltpu.roll(pltpu.roll(a, N - 16 * bit, 2), bit, 1)
            a = jnp.where(same, a, jnp.where((row & bit) == 0, up, down))
    return a.reshape(N, N)


def every(ref, j, count):
    return ref[pl.ds(j, N, count), :]


def pencil_to_rows(v, z_fwd, out):
    turned = jnp.concatenate([v[c * N : (c + 1) * N, :].T for c in range(3)], axis=1)
    waves = apply_left(z_fwd[...], turned)
    for part in range(2):
        for c in range(3):
            out[pl.ds(part * 3 + c, N, 6), :] = waves[part * N : (part + 1) * N, c * N : (c + 1) * N]


def rows_to_pencil(rows, z_inv, out):
    stack = jnp.concatenate(
        [jnp.concatenate([every(rows, part * 3 + c, 6) for c in range(3)], axis=1) for part in range(2)], axis=0
    )
    cells = apply_left(z_inv[...], stack)
    for c in range(3):
        out[c * N : (c + 1) * N, :] = cells[:, c * N : (c + 1) * N].T


def y_forward(pairs, mask, table):
    spectrum = apply_right(jnp.concatenate([jnp.concatenate(p, axis=1) for p in pairs], axis=0), table)
    real, imaginary = 0.0, 0.0
    for c in range(3):
        block = spectrum[c * N : (c + 1) * N]
        real = real + turn(block[:, :N] * mask, c)
        imaginary = imaginary + turn(block[:, N:] * mask, c)
    return real, imaginary


def y_inverse(pairs, mask, table):
    stack = [
        jnp.concatenate([turn(part, -c) * mask for part in pair], axis=1) for pair in pairs for c in range(3)
    ]
    return apply_right(jnp.concatenate(stack, axis=0), table)


def slab(rows, mask, z_fwd, z_inv, y_fwd, y_inv, out):
    mask = mask[...]
    pairs = [(every(rows, 2 * j, 4), every(rows, 2 * j + 1, 4)) for j in range(2)]
    lines = y_inverse(pairs, mask, y_inv[...])
    fields = [lines[f * N : (f + 1) * N] for f in range(6)]
    stack = jnp.concatenate(
        [jnp.concatenate([a[:, part * N : (part + 1) * N] for a in fields], axis=1) for part in range(2)], axis=0
    )
    grid = apply_left(z_inv[...], stack)
    u = [grid[:, c * N : (c + 1) * N] for c in range(3)]
    w = [grid[:, (3 + c) * N : (4 + c) * N] for c in range(3)]
    product = jnp.concatenate(
        [u[1] * w[2] - u[2] * w[1], u[2] * w[0] - u[0] * w[2], u[0] * w[1] - u[1] * w[0]], axis=1
    )
    waves = apply_left(z_fwd[...], product)
    pairs = [(waves[:N, c * N : (c + 1) * N], waves[N:, c * N : (c + 1) * N]) for c in range(3)]
    real, imaginary = y_forward(pairs, mask, y_fwd[...])
    out[pl.ds(0, N, 2), :] = real
    out[pl.ds(1, N, 2), :] = imaginary


class Waves:
    def __init__(self, lanes):
        kx = (lax.broadcasted_iota(jnp.int32, (KX, N), 0) - 42).astype(f32)

        def lane(i):
            return lanes[i : i + 1, :]

        self.own = kx * lane(0) + lane(1)
        self.after = kx * lane(2) + lane(3)
        self.before = kx * lane(4) + lane(5)
        self.squared = kx * kx + lane(6)
        self.inverse = 1.0 / jnp.where(self.squared > 0, self.squared, 1.0)
        self.scale = lane(7)
        self.is_last = jnp.broadcast_to(lane(8), (KX, N)) > 0
        self.is_first = jnp.broadcast_to(lane(9), (KX, N)) > 0
        self.third = lane(10)

    def project(self, part):
        part = part * self.scale
        along = part * self.own
        along = along + turn(along, 1)
        along = along + turn(along, 2)
        return part - self.own * (along * self.inverse)

    def cross(self, part):
        two = turn(part, 2)
        after = jnp.where(self.is_last, two, turn(part, -1))
        before = jnp.where(self.is_first, two, turn(part, 1))
        return self.after * before - self.before * after


def x_forward(real, imaginary, table):
    waves = apply_left(table, jnp.concatenate([real, imaginary], axis=0))
    return waves[:KX], waves[KX:]


def send_fields(waves, state, x_inv, out):
    curl = (-waves.cross(state[1]), waves.cross(state[0]))
    stack = jnp.concatenate([jnp.concatenate([state[i], curl[i]], axis=1) for i in range(2)], axis=0)
    lines = apply_left(x_inv[...], stack, 64)
    for field in range(2):
        for part in range(2):
            out[pl.ds(2 * field + part, N, 4), :] = lines[part * N : (part + 1) * N, field * N : (field + 1) * N]


def start_modes(rows, lanes, y_fwd, x_fwd, x_inv, out, state_out):
    waves = Waves(lanes)
    planes = [swap_blocks(every(rows, j, 6)) for j in range(6)]
    real, imaginary = y_forward([(planes[c], planes[3 + c]) for c in range(3)], waves.third, y_fwd[...])
    state = [waves.project(part) for part in x_forward(real, imaginary, x_fwd[...])]
    for i in range(2):
        state_out[i * KX : (i + 1) * KX, :] = state[i]
    send_fields(waves, state, x_inv, out)


def tendency(waves, rows, x_fwd, state):
    parts = x_forward(every(rows, 0, 2), every(rows, 1, 2), x_fwd[...])
    viscous = waves.squared * (1.0 / N)
    return [waves.project(parts[i]) - viscous * state[i] for i in range(2)]


def middle_modes(rows, lanes, x_fwd, x_inv, state_in, out, middle_out, half_out):
    waves = Waves(lanes)
    state = [state_in[i * KX : (i + 1) * KX, :] for i in range(2)]
    first = tendency(waves, rows, x_fwd, state)
    step = 2.0 / N
    middle = [state[i] + step * first[i] for i in range(2)]
    for i in range(2):
        middle_out[i * KX : (i + 1) * KX, :] = middle[i]
        half_out[i * KX : (i + 1) * KX, :] = state[i] + 0.5 * step * first[i]
    send_fields(waves, middle, x_inv, out)


def final_modes(rows, lanes, x_fwd, x_inv, y_inv, middle_in, half_in, out):
    waves = Waves(lanes)
    middle = [middle_in[i * KX : (i + 1) * KX, :] for i in range(2)]
    second = tendency(waves, rows, x_fwd, middle)
    final = [half_in[i * KX : (i + 1) * KX, :] + (1.0 / N) * second[i] for i in range(2)]
    lines = apply_left(x_inv[...], jnp.concatenate(final, axis=0), 64)
    cells = y_inverse([(lines[:N], lines[N:])], waves.third, y_inv[...])
    for c in range(3):
        for part in range(2):
            plane = cells[c * N : (c + 1) * N, part * N : (part + 1) * N]
            out[pl.ds(part * 3 + c, N, 6), :] = swap_blocks(plane)


def call(kernel, outs, last=False):
    shapes = [jax.ShapeDtypeStruct(s, f32) if last else pltpu.VMEM(s, f32) for s in outs]
    run = pl.pallas_call(kernel, out_shape=shapes if len(shapes) > 1 else shapes[0], name=kernel.__name__)
    return lambda *args: run(*[pltpu.with_memory_space_constraint(a, pltpu.VMEM) for a in args])


def exchange(rows):
    count = rows.shape[0] // N
    rows = rows.reshape(N, 1, count * N)
    rows = lax.all_to_all(rows, ("row", "col"), split_axis=0, concat_axis=0, tiled=True)
    return rows.reshape(N * count, N)


TABLES = tables()


def local(velocity):
    t = {name: jnp.asarray(value) for name, value in TABLES.items()}
    device = lax.axis_index("row") * lax.axis_size("col") + lax.axis_index("col")
    lanes = lax.dynamic_index_in_dim(t["lanes"], device, 0, keepdims=False)
    kept = (2 * KX, N)

    def physical(rows):
        return call(slab, [(2 * N, N)])(rows, t["mask"], t["z_fwd"], t["z_inv"], t["y_fwd"], t["y_inv"])

    shape = velocity.shape
    rows = exchange(call(pencil_to_rows, [(6 * N, N)])(velocity.reshape(3 * N, N), t["z_fwd"]))
    rows, state = call(start_modes, [(4 * N, N), kept])(rows, lanes, t["y_fwd"], t["x_fwd"], t["x_inv"])
    rows = exchange(physical(exchange(rows)))
    rows, middle, half = call(middle_modes, [(4 * N, N), kept, kept])(rows, lanes, t["x_fwd"], t["x_inv"], state)
    rows = exchange(physical(exchange(rows)))
    rows = call(final_modes, [(6 * N, N)])(rows, lanes, t["x_fwd"], t["x_inv"], t["y_inv"], middle, half)
    return call(rows_to_pencil, [(3 * N, N)], last=True)(exchange(rows), t["z_inv"]).reshape(shape)


def solution(mesh):
    placed = P(None, "row", "col", None)
    return jax.shard_map(local, mesh=mesh, in_specs=(placed,), out_specs=placed, check_vma=False)
```

```python
import jax
import jax.numpy as jnp
import ml_dtypes
import numpy as np
from jax import lax
from jax.experimental import pallas as pl
from jax.experimental.pallas import tpu as pltpu
from jax.sharding import PartitionSpec as P

N = 128
KX = 96
SLOTS = 32
f32, bf16 = jnp.float32, jnp.bfloat16


def owners():
    kz = np.array([1 + d // 3 for d in range(126)] + [0, 0])
    third = np.array([d % 3 for d in range(126)] + [0, 1])
    ky = np.zeros((4, SLOTS), np.int64)
    ok = np.zeros((4, SLOTS), bool)
    ky[0], ok[0] = np.arange(32), True
    ky[1], ok[1] = np.concatenate([np.arange(32, 43), np.arange(-42, -21)]), True
    ky[2, :21], ok[2, :21] = np.arange(-21, 0), True
    return kz, third, ky, ok


def split(a):
    hi = a.astype(np.float32).astype(ml_dtypes.bfloat16)
    lo = (a - hi.astype(np.float64)).astype(np.float32).astype(ml_dtypes.bfloat16)
    return hi, lo


def left(a, pad=0):
    hi, lo = split(a)
    zero = np.zeros((a.shape[0], pad), hi.dtype)
    return np.concatenate([hi, hi, lo, zero], axis=1)


def right(a):
    hi, lo = split(a)
    return np.concatenate([hi, hi, lo], axis=0)


def tables():
    kz, third, ky, ok = owners()
    cell = np.arange(N)

    def angle(a, b):
        return 2 * np.pi * (np.multiply.outer(a, b) % N) / N

    az = angle(kz, cell)
    z_fwd = left(np.concatenate([np.cos(az), -np.sin(az)], axis=0))
    z_inv = left(np.concatenate([np.cos(az.T), -np.sin(az.T)], axis=1))
    ay = angle(ky.reshape(-1), cell)
    keep = ok.reshape(-1)[:, None]
    cy, sy = np.cos(ay) * keep, np.sin(ay) * keep
    y_inv = right(np.block([[cy, sy], [-sy, cy]]))
    y_fwd = right(np.block([[cy.T, -sy.T], [sy.T, cy.T]]))
    ax = angle(np.arange(KX) - 42, cell)
    keep = (np.arange(KX) < 85)[:, None]
    cx, sx = np.cos(ax) * keep, np.sin(ax) * keep
    x_fwd = left(np.block([[cx, sx], [-sx, cx]]))
    x_inv = left(np.block([[cx.T, -sx.T], [sx.T, cx.T]]), 64)
    mask = (np.repeat(np.arange(4), SLOTS)[None, :] == third[:, None]).astype(np.float32)
    return dict(z_fwd=z_fwd, z_inv=z_inv, y_fwd=y_fwd, y_inv=y_inv, x_fwd=x_fwd, x_inv=x_inv, mask=mask)


def halves(a):
    hi = a.astype(bf16)
    return hi, (a - hi.astype(f32)).astype(bf16)


def dot(a, b):
    return jnp.dot(a, b, preferred_element_type=f32)


def apply_left(table, rows, pad=0):
    hi, lo = halves(rows)
    stack = [hi, lo, hi]
    if pad:
        stack.append(jnp.zeros((pad, rows.shape[1]), bf16))
    return dot(table, jnp.concatenate(stack, axis=0))


def apply_right(columns, table):
    hi, lo = halves(columns)
    return dot(jnp.concatenate([hi, lo, hi], axis=1), table)


def turn(a, groups):
    shift = (groups * SLOTS) % N
    return pltpu.roll(a, shift, 1) if shift else a


def swap_blocks(a):
    a = a.reshape(16, 8, N)
    row = lax.broadcasted_iota(jnp.int32, a.shape, 1)
    block = lax.broadcasted_iota(jnp.int32, a.shape, 2) // 16
    for bit in (4, 2, 1):
        same = (row & bit) == (block & bit)
        up = pltpu.roll(pltpu.roll(a, 16 * bit, 2), 8 - bit, 1)
        if bit == 4:
            a = jnp.where(same, a, up)
        else:
            down = pltpu.roll(pltpu.roll(a, N - 16 * bit, 2), bit, 1)
            a = jnp.where(same, a, jnp.where((row & bit) == 0, up, down))
    return a.reshape(N, N)


def every(ref, j, count):
    return ref[pl.ds(j, N, count), :]


def pencil_to_rows(v, z_fwd, out):
    turned = jnp.concatenate([v[c * N : (c + 1) * N, :].T for c in range(3)], axis=1)
    waves = apply_left(z_fwd[...], turned)
    for part in range(2):
        for c in range(3):
            out[pl.ds(part * 3 + c, N, 6), :] = waves[part * N : (part + 1) * N, c * N : (c + 1) * N]


def rows_to_pencil(rows, z_inv, out):
    stack = jnp.concatenate(
        [jnp.concatenate([every(rows, part * 3 + c, 6) for c in range(3)], axis=1) for part in range(2)], axis=0
    )
    cells = apply_left(z_inv[...], stack)
    for c in range(3):
        out[c * N : (c + 1) * N, :] = cells[:, c * N : (c + 1) * N].T


def y_forward(pairs, mask, table):
    spectrum = apply_right(jnp.concatenate([jnp.concatenate(p, axis=1) for p in pairs], axis=0), table)
    real, imaginary = 0.0, 0.0
    for c in range(3):
        block = spectrum[c * N : (c + 1) * N]
        real = real + turn(block[:, :N] * mask, c)
        imaginary = imaginary + turn(block[:, N:] * mask, c)
    return real, imaginary


def y_inverse(pairs, mask, table):
    stack = [
        jnp.concatenate([turn(part, -c) * mask for part in pair], axis=1) for pair in pairs for c in range(3)
    ]
    return apply_right(jnp.concatenate(stack, axis=0), table)


def slab(rows, mask, z_fwd, z_inv, y_fwd, y_inv, out):
    mask = mask[...]
    pairs = [(every(rows, 2 * j, 4), every(rows, 2 * j + 1, 4)) for j in range(2)]
    lines = y_inverse(pairs, mask, y_inv[...])
    fields = [lines[f * N : (f + 1) * N] for f in range(6)]
    stack = jnp.concatenate(
        [jnp.concatenate([a[:, part * N : (part + 1) * N] for a in fields], axis=1) for part in range(2)], axis=0
    )
    grid = apply_left(z_inv[...], stack)
    u = [grid[:, c * N : (c + 1) * N] for c in range(3)]
    w = [grid[:, (3 + c) * N : (4 + c) * N] for c in range(3)]
    product = jnp.concatenate(
        [u[1] * w[2] - u[2] * w[1], u[2] * w[0] - u[0] * w[2], u[0] * w[1] - u[1] * w[0]], axis=1
    )
    waves = apply_left(z_fwd[...], product)
    pairs = [(waves[:N, c * N : (c + 1) * N], waves[N:, c * N : (c + 1) * N]) for c in range(3)]
    real, imaginary = y_forward(pairs, mask, y_fwd[...])
    out[pl.ds(0, N, 2), :] = real
    out[pl.ds(1, N, 2), :] = imaginary


class Waves:
    def __init__(self):
        device = lax.axis_index("row") * lax.axis_size("col") + lax.axis_index("col")
        kz = jnp.where(device < 126, 1 + lax.div(device, 3), 0)
        third = jnp.where(device < 126, lax.rem(device, 3), device - 126)
        lane = lax.broadcasted_iota(jnp.int32, (1, N), 1)
        group, slot = lane // SLOTS, lane % SLOTS
        c = (group - third + 4) % 4
        wrapped = jnp.where(slot < 11, slot + 32, slot - 53)
        ky = jnp.where(third == 0, slot, jnp.where(third == 1, wrapped, slot - 21))
        good = (c < 3) & ((third < 2) | (slot < 21)) & ((kz > 0) | (ky >= 0))
        count = jnp.where((kz == 0) & (ky == 0), 1.0, 2.0)
        kx = lax.broadcasted_iota(jnp.int32, (KX, N), 0) - 42

        def component(x, y, z):
            return jnp.where(c == x, kx, jnp.where(c == y, ky, jnp.where(c == z, kz, 0))).astype(f32)

        self.own = component(0, 1, 2)
        self.after = component(2, 0, 1)
        self.before = component(1, 2, 0)
        self.squared = (kx * kx + (ky * ky + kz * kz)).astype(f32)
        self.inverse = 1.0 / jnp.where(self.squared > 0, self.squared, 1.0)
        self.scale = jnp.where(good, count * (1.0 / N**3), 0.0)
        whole = jnp.broadcast_to(c, (KX, N))
        self.is_last = whole == 2
        self.is_first = whole == 0
        self.third = (group == third).astype(f32)

    def project(self, part):
        part = part * self.scale
        along = part * self.own
        along = along + turn(along, 1)
        along = along + turn(along, 2)
        return part - self.own * (along * self.inverse)

    def cross(self, part):
        two = turn(part, 2)
        after = jnp.where(self.is_last, two, turn(part, -1))
        before = jnp.where(self.is_first, two, turn(part, 1))
        return self.after * before - self.before * after


def x_forward(real, imaginary, table):
    waves = apply_left(table, jnp.concatenate([real, imaginary], axis=0))
    return waves[:KX], waves[KX:]


def send_fields(waves, state, x_inv, out):
    curl = (-waves.cross(state[1]), waves.cross(state[0]))
    stack = jnp.concatenate([jnp.concatenate([state[i], curl[i]], axis=1) for i in range(2)], axis=0)
    lines = apply_left(x_inv[...], stack, 64)
    for field in range(2):
        for part in range(2):
            out[pl.ds(2 * field + part, N, 4), :] = lines[part * N : (part + 1) * N, field * N : (field + 1) * N]


def start_modes(rows, y_fwd, x_fwd, x_inv, out, state_out):
    waves = Waves()
    planes = [swap_blocks(every(rows, j, 6)) for j in range(6)]
    real, imaginary = y_forward([(planes[c], planes[3 + c]) for c in range(3)], waves.third, y_fwd[...])
    state = [waves.project(part) for part in x_forward(real, imaginary, x_fwd[...])]
    for i in range(2):
        state_out[i * KX : (i + 1) * KX, :] = state[i]
    send_fields(waves, state, x_inv, out)


def tendency(waves, rows, x_fwd, state):
    parts = x_forward(every(rows, 0, 2), every(rows, 1, 2), x_fwd[...])
    viscous = waves.squared * (1.0 / N)
    return [waves.project(parts[i]) - viscous * state[i] for i in range(2)]


def middle_modes(rows, x_fwd, x_inv, state_in, out, middle_out, half_out):
    waves = Waves()
    state = [state_in[i * KX : (i + 1) * KX, :] for i in range(2)]
    first = tendency(waves, rows, x_fwd, state)
    step = 2.0 / N
    middle = [state[i] + step * first[i] for i in range(2)]
    for i in range(2):
        middle_out[i * KX : (i + 1) * KX, :] = middle[i]
        half_out[i * KX : (i + 1) * KX, :] = state[i] + 0.5 * step * first[i]
    send_fields(waves, middle, x_inv, out)


def final_modes(rows, x_fwd, x_inv, y_inv, middle_in, half_in, out):
    waves = Waves()
    middle = [middle_in[i * KX : (i + 1) * KX, :] for i in range(2)]
    second = tendency(waves, rows, x_fwd, middle)
    final = [half_in[i * KX : (i + 1) * KX, :] + (1.0 / N) * second[i] for i in range(2)]
    lines = apply_left(x_inv[...], jnp.concatenate(final, axis=0), 64)
    cells = y_inverse([(lines[:N], lines[N:])], waves.third, y_inv[...])
    for c in range(3):
        for part in range(2):
            plane = cells[c * N : (c + 1) * N, part * N : (part + 1) * N]
            out[pl.ds(part * 3 + c, N, 6), :] = swap_blocks(plane)


def call(kernel, outs, last=False):
    shapes = [jax.ShapeDtypeStruct(s, f32) if last else pltpu.VMEM(s, f32) for s in outs]
    run = pl.pallas_call(kernel, out_shape=shapes if len(shapes) > 1 else shapes[0], name=kernel.__name__)
    return lambda *args: run(*[pltpu.with_memory_space_constraint(a, pltpu.VMEM) for a in args])


def exchange(rows):
    count = rows.shape[0] // N
    rows = rows.reshape(N, 1, count * N)
    rows = lax.all_to_all(rows, ("row", "col"), split_axis=0, concat_axis=0, tiled=True)
    return rows.reshape(N * count, N)


TABLES = tables()


def local(velocity):
    t = {name: jnp.asarray(value) for name, value in TABLES.items()}
    kept = (2 * KX, N)

    def physical(rows):
        return call(slab, [(2 * N, N)])(rows, t["mask"], t["z_fwd"], t["z_inv"], t["y_fwd"], t["y_inv"])

    shape = velocity.shape
    rows = exchange(call(pencil_to_rows, [(6 * N, N)])(velocity.reshape(3 * N, N), t["z_fwd"]))
    rows, state = call(start_modes, [(4 * N, N), kept])(rows, t["y_fwd"], t["x_fwd"], t["x_inv"])
    rows = exchange(physical(exchange(rows)))
    rows, middle, half = call(middle_modes, [(4 * N, N), kept, kept])(rows, t["x_fwd"], t["x_inv"], state)
    rows = exchange(physical(exchange(rows)))
    rows = call(final_modes, [(6 * N, N)])(rows, t["x_fwd"], t["x_inv"], t["y_inv"], middle, half)
    return call(rows_to_pencil, [(3 * N, N)], last=True)(exchange(rows), t["z_inv"]).reshape(shape)


def solution(mesh):
    placed = P(None, "row", "col", None)
    return jax.shard_map(local, mesh=mesh, in_specs=(placed,), out_specs=placed, check_vma=False)
```

```python
import jax
import jax.numpy as jnp
import ml_dtypes
import numpy as np
from jax import lax
from jax.experimental import pallas as pl
from jax.experimental.pallas import tpu as pltpu
from jax.sharding import PartitionSpec as P

N = 128
KX = 96
SLOTS = 32
f32, bf16 = jnp.float32, jnp.bfloat16


def owners():
    kz = np.array([1 + d // 3 for d in range(126)] + [0, 0])
    third = np.array([d % 3 for d in range(126)] + [0, 1])
    ky = np.zeros((4, SLOTS), np.int64)
    ok = np.zeros((4, SLOTS), bool)
    ky[0], ok[0] = np.arange(32), True
    ky[1], ok[1] = np.concatenate([np.arange(32, 43), np.arange(-42, -21)]), True
    ky[2, :21], ok[2, :21] = np.arange(-21, 0), True
    return kz, third, ky, ok


def split(a):
    hi = a.astype(np.float32).astype(ml_dtypes.bfloat16)
    lo = (a - hi.astype(np.float64)).astype(np.float32).astype(ml_dtypes.bfloat16)
    return hi, lo


def left(a, pad=0):
    hi, lo = split(a)
    zero = np.zeros((a.shape[0], pad), hi.dtype)
    return np.concatenate([hi, hi, lo, zero], axis=1)


def right(a):
    hi, lo = split(a)
    return np.concatenate([hi, hi, lo], axis=0)


def tables():
    kz, third, ky, ok = owners()
    cell = np.arange(N)

    def angle(a, b):
        return 2 * np.pi * (np.multiply.outer(a, b) % N) / N

    az = angle(kz, cell)
    z_fwd = left(np.concatenate([np.cos(az), -np.sin(az)], axis=0))
    z_inv = left(np.concatenate([np.cos(az.T), -np.sin(az.T)], axis=1))
    ay = angle(ky.reshape(-1), cell)
    keep = ok.reshape(-1)[:, None]
    cy, sy = np.cos(ay) * keep, np.sin(ay) * keep
    y_inv = right(np.block([[cy, sy], [-sy, cy]]))
    y_fwd = right(np.block([[cy.T, -sy.T], [sy.T, cy.T]]))
    ax = angle(np.arange(KX) - 42, cell)
    keep = (np.arange(KX) < 85)[:, None]
    cx, sx = np.cos(ax) * keep, np.sin(ax) * keep
    x_fwd = left(np.block([[cx, sx], [-sx, cx]]))
    x_inv = left(np.block([[cx.T, -sx.T], [sx.T, cx.T]]), 64)
    mask = (np.repeat(np.arange(4), SLOTS)[None, :] == third[:, None]).astype(np.float32)
    return dict(z_fwd=z_fwd, z_inv=z_inv, y_fwd=y_fwd, y_inv=y_inv, x_fwd=x_fwd, x_inv=x_inv, mask=mask)


def halves(a):
    hi = a.astype(bf16)
    return hi, (a - hi.astype(f32)).astype(bf16)


def dot(a, b):
    return jnp.dot(a, b, preferred_element_type=f32)


def apply_left(table, rows, pad=0):
    hi, lo = halves(rows)
    stack = [hi, lo, hi]
    if pad:
        stack.append(jnp.zeros((pad, rows.shape[1]), bf16))
    return dot(table, jnp.concatenate(stack, axis=0))


def apply_right(columns, table):
    hi, lo = halves(columns)
    return dot(jnp.concatenate([hi, lo, hi], axis=1), table)


def turn(a, groups):
    shift = (groups * SLOTS) % N
    return pltpu.roll(a, shift, 1) if shift else a


def swap_blocks(a):
    a = a.reshape(16, 8, N)
    row = lax.broadcasted_iota(jnp.int32, a.shape, 1)
    block = lax.broadcasted_iota(jnp.int32, a.shape, 2) // 16
    for bit in (4, 2, 1):
        same = (row & bit) == (block & bit)
        up = pltpu.roll(pltpu.roll(a, 16 * bit, 2), 8 - bit, 1)
        if bit == 4:
            a = jnp.where(same, a, up)
        else:
            down = pltpu.roll(pltpu.roll(a, N - 16 * bit, 2), bit, 1)
            a = jnp.where(same, a, jnp.where((row & bit) == 0, up, down))
    return a.reshape(N, N)


def every(ref, j, count):
    return ref[pl.ds(j, N, count), :]


def pencil_to_rows(v_hbm, z_hbm, out, v, z_fwd, arrived):
    copies = [pltpu.make_async_copy(z_hbm, z_fwd, arrived.at[3])]
    for c in range(3):
        part = pl.ds(c * N, N)
        copies.append(pltpu.make_async_copy(v_hbm.at[part, :], v.at[part, :], arrived.at[c]))
    for copy in copies:
        copy.start()
    copies[0].wait()
    for c in range(3):
        copies[1 + c].wait()
        waves = apply_left(z_fwd[...], v[c * N : (c + 1) * N, :].T)
        for part in range(2):
            out[pl.ds(part * 3 + c, N, 6), :] = waves[part * N : (part + 1) * N]


def rows_to_pencil(rows, z_inv, out):
    stack = jnp.concatenate(
        [jnp.concatenate([every(rows, part * 3 + c, 6) for c in range(3)], axis=1) for part in range(2)], axis=0
    )
    cells = apply_left(z_inv[...], stack)
    for c in range(3):
        out[c * N : (c + 1) * N, :] = cells[:, c * N : (c + 1) * N].T


def y_forward(pairs, mask, table):
    spectrum = apply_right(jnp.concatenate([jnp.concatenate(p, axis=1) for p in pairs], axis=0), table)
    real, imaginary = 0.0, 0.0
    for c in range(3):
        block = spectrum[c * N : (c + 1) * N]
        real = real + turn(block[:, :N] * mask, c)
        imaginary = imaginary + turn(block[:, N:] * mask, c)
    return real, imaginary


def y_inverse(places, mask, table):
    stack = [jnp.concatenate([turn(a, -group) * mask for a, group in pair], axis=1) for pair in places]
    return apply_right(jnp.concatenate(stack, axis=0), table)


def slab(rows, mask, z_fwd, z_inv, y_fwd, y_inv, out):
    mask = mask[...]
    real, imaginary, rest = (every(rows, j, 3) for j in range(3))
    places = [((real, f), (imaginary, f)) for f in range(4)] + [((rest, f), (rest, f + 2)) for f in (1, 2)]
    lines = y_inverse(places, mask, y_inv[...])
    fields = [lines[f * N : (f + 1) * N] for f in range(6)]
    stack = jnp.concatenate(
        [jnp.concatenate([a[:, part * N : (part + 1) * N] for a in fields], axis=1) for part in range(2)], axis=0
    )
    grid = apply_left(z_inv[...], stack)
    u = [grid[:, c * N : (c + 1) * N] for c in range(3)]
    w = [grid[:, (3 + c) * N : (4 + c) * N] for c in range(3)]
    product = jnp.concatenate(
        [u[1] * w[2] - u[2] * w[1], u[2] * w[0] - u[0] * w[2], u[0] * w[1] - u[1] * w[0]], axis=1
    )
    waves = apply_left(z_fwd[...], product)
    pairs = [(waves[:N, c * N : (c + 1) * N], waves[N:, c * N : (c + 1) * N]) for c in range(3)]
    real, imaginary = y_forward(pairs, mask, y_fwd[...])
    out[pl.ds(0, N, 2), :] = real
    out[pl.ds(1, N, 2), :] = imaginary


class Waves:
    def __init__(self):
        device = lax.axis_index("row") * lax.axis_size("col") + lax.axis_index("col")
        kz = jnp.where(device < 126, 1 + lax.div(device, 3), 0)
        third = jnp.where(device < 126, lax.rem(device, 3), device - 126)
        lane = lax.broadcasted_iota(jnp.int32, (1, N), 1)
        group, slot = lane // SLOTS, lane % SLOTS
        c = (group - third + 4) % 4
        wrapped = jnp.where(slot < 11, slot + 32, slot - 53)
        ky = jnp.where(third == 0, slot, jnp.where(third == 1, wrapped, slot - 21))
        good = (c < 3) & ((third < 2) | (slot < 21)) & ((kz > 0) | (ky >= 0))
        count = jnp.where((kz == 0) & (ky == 0), 1.0, 2.0)
        kx = lax.broadcasted_iota(jnp.int32, (KX, N), 0) - 42

        def component(x, y, z):
            return jnp.where(c == x, kx, jnp.where(c == y, ky, jnp.where(c == z, kz, 0))).astype(f32)

        self.own = component(0, 1, 2)
        self.after = component(2, 0, 1)
        self.before = component(1, 2, 0)
        self.squared = (kx * kx + (ky * ky + kz * kz)).astype(f32)
        self.inverse = 1.0 / jnp.where(self.squared > 0, self.squared, 1.0)
        self.scale = jnp.where(good, count * (1.0 / N**3), 0.0)
        whole = jnp.broadcast_to(c, (KX, N))
        self.is_last = whole == 2
        self.is_first = whole == 0
        self.is_free = whole == 3
        lines = jnp.broadcast_to(c, (N, N))
        self.has_rest = (lines == 1) | (lines == 2)
        self.third = (group == third).astype(f32)

    def project(self, part):
        part = part * self.scale
        along = part * self.own
        along = along + turn(along, 1)
        along = along + turn(along, 2)
        return part - self.own * (along * self.inverse)

    def cross(self, part):
        two = turn(part, 2)
        after = jnp.where(self.is_last, two, turn(part, -1))
        before = jnp.where(self.is_first, two, turn(part, 1))
        return self.after * before - self.before * after


def x_forward(real, imaginary, table):
    waves = apply_left(table, jnp.concatenate([real, imaginary], axis=0))
    return waves[:KX], waves[KX:]


def send_fields(waves, state, x_inv, out):
    curl = (-waves.cross(state[1]), waves.cross(state[0]))
    both = [jnp.where(waves.is_free, turn(curl[i], 3), state[i]) for i in range(2)]
    stack = jnp.concatenate([jnp.concatenate([both[i], curl[i]], axis=1) for i in range(2)], axis=0)
    lines = apply_left(x_inv[...], stack, 64)
    for part in range(2):
        out[pl.ds(part, N, 3), :] = lines[part * N : (part + 1) * N, :N]
    out[pl.ds(2, N, 3), :] = jnp.where(waves.has_rest, lines[:N, N:], turn(lines[N:, N:], 2))


def start_modes(rows, y_fwd, x_fwd, x_inv, out, state_out):
    waves = Waves()
    planes = [swap_blocks(every(rows, j, 6)) for j in range(6)]
    real, imaginary = y_forward([(planes[c], planes[3 + c]) for c in range(3)], waves.third, y_fwd[...])
    state = [waves.project(part) for part in x_forward(real, imaginary, x_fwd[...])]
    for i in range(2):
        state_out[i * KX : (i + 1) * KX, :] = state[i]
    send_fields(waves, state, x_inv, out)


def tendency(waves, rows, x_fwd, state):
    parts = x_forward(every(rows, 0, 2), every(rows, 1, 2), x_fwd[...])
    viscous = waves.squared * (1.0 / N)
    return [waves.project(parts[i]) - viscous * state[i] for i in range(2)]


def middle_modes(rows, x_fwd, x_inv, state_in, out, middle_out, half_out):
    waves = Waves()
    state = [state_in[i * KX : (i + 1) * KX, :] for i in range(2)]
    first = tendency(waves, rows, x_fwd, state)
    step = 2.0 / N
    middle = [state[i] + step * first[i] for i in range(2)]
    for i in range(2):
        middle_out[i * KX : (i + 1) * KX, :] = middle[i]
        half_out[i * KX : (i + 1) * KX, :] = state[i] + 0.5 * step * first[i]
    send_fields(waves, middle, x_inv, out)


def final_modes(rows, x_fwd, x_inv, y_inv, middle_in, half_in, out):
    waves = Waves()
    middle = [middle_in[i * KX : (i + 1) * KX, :] for i in range(2)]
    second = tendency(waves, rows, x_fwd, middle)
    final = [half_in[i * KX : (i + 1) * KX, :] + (1.0 / N) * second[i] for i in range(2)]
    lines = apply_left(x_inv[...], jnp.concatenate(final, axis=0), 64)
    cells = y_inverse([((lines[:N], c), (lines[N:], c)) for c in range(3)], waves.third, y_inv[...])
    for c in range(3):
        for part in range(2):
            plane = cells[c * N : (c + 1) * N, part * N : (part + 1) * N]
            out[pl.ds(part * 3 + c, N, 6), :] = swap_blocks(plane)


def call(kernel, outs, last=False):
    shapes = [jax.ShapeDtypeStruct(s, f32) if last else pltpu.VMEM(s, f32) for s in outs]
    run = pl.pallas_call(kernel, out_shape=shapes if len(shapes) > 1 else shapes[0], name=kernel.__name__)
    return lambda *args: run(*[pltpu.with_memory_space_constraint(a, pltpu.VMEM) for a in args])


def first_call(v, z_fwd):
    run = pl.pallas_call(
        pencil_to_rows,
        out_shape=pltpu.VMEM((6 * N, N), f32),
        in_specs=[pl.BlockSpec(memory_space=pl.ANY)] * 2,
        scratch_shapes=[pltpu.VMEM(v.shape, f32), pltpu.VMEM(z_fwd.shape, bf16), pltpu.SemaphoreType.DMA((4,))],
        name="pencil_to_rows",
    )
    return run(v, z_fwd)


def exchange(rows):
    count = rows.shape[0] // N
    rows = rows.reshape(N, 1, count * N)
    rows = lax.all_to_all(rows, ("row", "col"), split_axis=0, concat_axis=0, tiled=True)
    return rows.reshape(N * count, N)


TABLES = tables()


def local(velocity):
    t = {name: jnp.asarray(value) for name, value in TABLES.items()}
    kept = (2 * KX, N)

    def physical(rows):
        return call(slab, [(2 * N, N)])(rows, t["mask"], t["z_fwd"], t["z_inv"], t["y_fwd"], t["y_inv"])

    shape = velocity.shape
    rows = exchange(first_call(velocity.reshape(3 * N, N), t["z_fwd"]))
    rows, state = call(start_modes, [(3 * N, N), kept])(rows, t["y_fwd"], t["x_fwd"], t["x_inv"])
    rows = exchange(physical(exchange(rows)))
    rows, middle, half = call(middle_modes, [(3 * N, N), kept, kept])(rows, t["x_fwd"], t["x_inv"], state)
    rows = exchange(physical(exchange(rows)))
    rows = call(final_modes, [(6 * N, N)])(rows, t["x_fwd"], t["x_inv"], t["y_inv"], middle, half)
    return call(rows_to_pencil, [(3 * N, N)], last=True)(exchange(rows), t["z_inv"]).reshape(shape)


def solution(mesh):
    placed = P(None, "row", "col", None)
    return jax.shard_map(local, mesh=mesh, in_specs=(placed,), out_specs=placed, check_vma=False)
```

```python
import jax
import jax.numpy as jnp
import ml_dtypes
import numpy as np
from jax import lax
from jax.experimental import pallas as pl
from jax.experimental.pallas import tpu as pltpu
from jax.sharding import PartitionSpec as P

N = 128
KX = 96
SLOTS = 32
f32, bf16 = jnp.float32, jnp.bfloat16


def owners():
    kz = np.array([1 + d // 3 for d in range(126)] + [0, 0])
    third = np.array([d % 3 for d in range(126)] + [0, 1])
    ky = np.zeros((4, SLOTS), np.int64)
    ok = np.zeros((4, SLOTS), bool)
    ky[0], ok[0] = np.arange(32), True
    ky[1], ok[1] = np.concatenate([np.arange(32, 43), np.arange(-42, -21)]), True
    ky[2, :21], ok[2, :21] = np.arange(-21, 0), True
    return kz, third, ky, ok


def split(a):
    hi = a.astype(np.float32).astype(ml_dtypes.bfloat16)
    lo = (a - hi.astype(np.float64)).astype(np.float32).astype(ml_dtypes.bfloat16)
    return hi, lo


def left(a, pad=0):
    hi, lo = split(a)
    zero = np.zeros((a.shape[0], pad), hi.dtype)
    return np.concatenate([hi, hi, lo, zero], axis=1)


def right(a):
    hi, lo = split(a)
    return np.concatenate([hi, hi, lo], axis=0)


def tables():
    kz, third, ky, ok = owners()
    cell = np.arange(N)

    def angle(a, b):
        return 2 * np.pi * (np.multiply.outer(a, b) % N) / N

    az = angle(kz, cell)
    z_fwd = left(np.concatenate([np.cos(az), -np.sin(az)], axis=0))
    z_inv = left(np.concatenate([np.cos(az.T), -np.sin(az.T)], axis=1))
    ay = angle(ky.reshape(-1), cell)
    keep = ok.reshape(-1)[:, None]
    cy, sy = np.cos(ay) * keep, np.sin(ay) * keep
    y_inv = right(np.block([[cy, sy], [-sy, cy]]))
    y_fwd = right(np.block([[cy.T, -sy.T], [sy.T, cy.T]]))
    ax = angle(np.arange(KX) - 42, cell)
    keep = (np.arange(KX) < 85)[:, None]
    cx, sx = np.cos(ax) * keep, np.sin(ax) * keep
    x_fwd = left(np.block([[cx, sx], [-sx, cx]]))
    x_inv = left(np.block([[cx.T, -sx.T], [sx.T, cx.T]]), 64)
    mask = (np.repeat(np.arange(4), SLOTS)[None, :] == third[:, None]).astype(np.float32)
    flip = np.arange(N) // 8 * 8 + (-np.arange(N)) % 8
    x_first = left(np.block([[cx, sx], [-sx, cx]])[:, np.concatenate([flip, N + flip])])
    back = (np.arange(N) // 16 * -16) % N + np.arange(N) % 16
    y_last = right(np.block([[cy, sy], [-sy, cy]])[:, np.concatenate([back, N + back])])
    return dict(x_first=x_first, y_last=y_last, z_fwd=z_fwd, z_inv=z_inv, y_fwd=y_fwd, y_inv=y_inv, x_fwd=x_fwd, x_inv=x_inv, mask=mask)


def halves(a):
    hi = a.astype(bf16)
    return hi, (a - hi.astype(f32)).astype(bf16)


def dot(a, b):
    return jnp.dot(a, b, preferred_element_type=f32)


def apply_left(table, rows, pad=0):
    hi, lo = halves(rows)
    stack = [hi, lo, hi]
    if pad:
        stack.append(jnp.zeros((pad, rows.shape[1]), bf16))
    return dot(table, jnp.concatenate(stack, axis=0))


def apply_right(columns, table):
    hi, lo = halves(columns)
    return dot(jnp.concatenate([hi, lo, hi], axis=1), table)


def turn(a, groups):
    shift = (groups * SLOTS) % N
    return pltpu.roll(a, shift, 1) if shift else a


def turn_blocks(a):
    block = (lax.broadcasted_iota(jnp.int32, (N, N), 1) // 16).reshape(16, 8, N)
    a = pltpu.roll(a, 0, 1, stride=16, stride_axis=0).reshape(16, 8, N)
    for bit in (1, 2, 4):
        a = jnp.where((block & bit) == 0, a, pltpu.roll(a, 8 - bit, 1))
    return pltpu.roll(a.reshape(N, N), 0, 1, stride=16, stride_axis=0)


def every(ref, j, count):
    return ref[pl.ds(j, N, count), :]


def pencil_to_rows(v_hbm, z_hbm, out, v, z_fwd, arrived):
    copies = [pltpu.make_async_copy(z_hbm, z_fwd, arrived.at[3])]
    for c in range(3):
        part = pl.ds(c * N, N)
        copies.append(pltpu.make_async_copy(v_hbm.at[part, :], v.at[part, :], arrived.at[c]))
    for copy in copies:
        copy.start()
    for copy in copies:
        copy.wait()
    turned = jnp.concatenate([v[c * N : (c + 1) * N, :].T for c in range(3)], axis=1)
    waves = apply_left(z_fwd[...], turned)
    for part in range(2):
        for c in range(3):
            out[pl.ds(part * 3 + c, N, 6), :] = waves[part * N : (part + 1) * N, c * N : (c + 1) * N]


def rows_to_pencil(rows, z_inv, out):
    stack = jnp.concatenate(
        [jnp.concatenate([every(rows, part * 3 + c, 6) for c in range(3)], axis=1) for part in range(2)], axis=0
    )
    cells = apply_left(z_inv[...], stack)
    for c in range(3):
        out[c * N : (c + 1) * N, :] = cells[:, c * N : (c + 1) * N].T


def y_forward(pairs, mask, table):
    real, imaginary = 0.0, 0.0
    for c in range(3):
        block = apply_right(jnp.concatenate(pairs[c], axis=1), table)
        real = real + turn(block[:, :N] * mask, c)
        imaginary = imaginary + turn(block[:, N:] * mask, c)
    return real, imaginary


def y_inverse(places, mask, table):
    stack = [jnp.concatenate([turn(a, -group) * mask for a, group in pair], axis=1) for pair in places]
    return apply_right(jnp.concatenate(stack, axis=0), table)


def slab(rows, mask, z_fwd, z_inv, y_fwd, y_inv, out):
    mask = mask[...]
    real, imaginary, rest = (every(rows, j, 3) for j in range(3))
    places = [((real, f), (imaginary, f)) for f in range(4)] + [((rest, f), (rest, f + 2)) for f in (1, 2)]
    lines = y_inverse(places, mask, y_inv[...])
    fields = [lines[f * N : (f + 1) * N] for f in range(6)]
    stack = jnp.concatenate(
        [jnp.concatenate([a[:, part * N : (part + 1) * N] for a in fields], axis=1) for part in range(2)], axis=0
    )
    grid = apply_left(z_inv[...], stack)
    u = [grid[:, c * N : (c + 1) * N] for c in range(3)]
    w = [grid[:, (3 + c) * N : (4 + c) * N] for c in range(3)]
    product = jnp.concatenate(
        [u[1] * w[2] - u[2] * w[1], u[2] * w[0] - u[0] * w[2], u[0] * w[1] - u[1] * w[0]], axis=1
    )
    waves = apply_left(z_fwd[...], product)
    pairs = [(waves[:N, c * N : (c + 1) * N], waves[N:, c * N : (c + 1) * N]) for c in range(3)]
    real, imaginary = y_forward(pairs, mask, y_fwd[...])
    out[pl.ds(0, N, 2), :] = real
    out[pl.ds(1, N, 2), :] = imaginary


class Waves:
    def __init__(self):
        device = lax.axis_index("row") * lax.axis_size("col") + lax.axis_index("col")
        kz = jnp.where(device < 126, 1 + lax.div(device, 3), 0)
        third = jnp.where(device < 126, lax.rem(device, 3), device - 126)
        lane = lax.broadcasted_iota(jnp.int32, (1, N), 1)
        group, slot = lane // SLOTS, lane % SLOTS
        c = (group - third + 4) % 4
        wrapped = jnp.where(slot < 11, slot + 32, slot - 53)
        ky = jnp.where(third == 0, slot, jnp.where(third == 1, wrapped, slot - 21))
        good = (c < 3) & ((third < 2) | (slot < 21)) & ((kz > 0) | (ky >= 0))
        count = jnp.where((kz == 0) & (ky == 0), 1.0, 2.0)
        kx = lax.broadcasted_iota(jnp.int32, (KX, N), 0) - 42

        def component(x, y, z):
            return jnp.where(c == x, kx, jnp.where(c == y, ky, jnp.where(c == z, kz, 0))).astype(f32)

        self.own = component(0, 1, 2)
        self.after = component(2, 0, 1)
        self.before = component(1, 2, 0)
        self.squared = (kx * kx + (ky * ky + kz * kz)).astype(f32)
        self.inverse = 1.0 / jnp.where(self.squared > 0, self.squared, 1.0)
        self.scale = jnp.where(good, count * (1.0 / N**3), 0.0)
        whole = jnp.broadcast_to(c, (KX, N))
        self.is_last = whole == 2
        self.is_first = whole == 0
        self.is_free = whole == 3
        lines = jnp.broadcast_to(c, (N, N))
        self.has_rest = (lines == 1) | (lines == 2)
        self.third = (group == third).astype(f32)

    def project(self, part):
        part = part * self.scale
        along = part * self.own
        along = along + turn(along, 1)
        along = along + turn(along, 2)
        return part - self.own * (along * self.inverse)

    def cross(self, part):
        two = turn(part, 2)
        after = jnp.where(self.is_last, two, turn(part, -1))
        before = jnp.where(self.is_first, two, turn(part, 1))
        return self.after * before - self.before * after


def x_forward(real, imaginary, table):
    waves = apply_left(table, jnp.concatenate([real, imaginary], axis=0))
    return waves[:KX], waves[KX:]


def send_fields(waves, state, x_inv, out):
    curl = (-waves.cross(state[1]), waves.cross(state[0]))
    both = [jnp.where(waves.is_free, turn(curl[i], 3), state[i]) for i in range(2)]
    stack = jnp.concatenate([jnp.concatenate([both[i], curl[i]], axis=1) for i in range(2)], axis=0)
    lines = apply_left(x_inv[...], stack, 64)
    for part in range(2):
        out[pl.ds(part, N, 3), :] = lines[part * N : (part + 1) * N, :N]
    out[pl.ds(2, N, 3), :] = jnp.where(waves.has_rest, lines[:N, N:], turn(lines[N:, N:], 2))


def start_modes(rows, y_fwd, x_fwd, x_inv, out, state_out):
    waves = Waves()
    planes = [turn_blocks(every(rows, j, 6)) for j in range(6)]
    real, imaginary = y_forward([(planes[c], planes[3 + c]) for c in range(3)], waves.third, y_fwd[...])
    state = [waves.project(part) for part in x_forward(real, imaginary, x_fwd[...])]
    for i in range(2):
        state_out[i * KX : (i + 1) * KX, :] = state[i]
    send_fields(waves, state, x_inv, out)


def tendency(waves, rows, x_fwd, state):
    parts = x_forward(every(rows, 0, 2), every(rows, 1, 2), x_fwd[...])
    viscous = waves.squared * (1.0 / N)
    return [waves.project(parts[i]) - viscous * state[i] for i in range(2)]


def middle_modes(rows, x_fwd, x_inv, state_in, out, middle_out, half_out):
    waves = Waves()
    state = [state_in[i * KX : (i + 1) * KX, :] for i in range(2)]
    first = tendency(waves, rows, x_fwd, state)
    step = 2.0 / N
    middle = [state[i] + step * first[i] for i in range(2)]
    for i in range(2):
        middle_out[i * KX : (i + 1) * KX, :] = middle[i]
        half_out[i * KX : (i + 1) * KX, :] = state[i] + 0.5 * step * first[i]
    send_fields(waves, middle, x_inv, out)


def final_modes(rows, x_fwd, x_inv, y_inv, middle_in, half_in, out):
    waves = Waves()
    middle = [middle_in[i * KX : (i + 1) * KX, :] for i in range(2)]
    second = tendency(waves, rows, x_fwd, middle)
    final = [half_in[i * KX : (i + 1) * KX, :] + (1.0 / N) * second[i] for i in range(2)]
    lines = apply_left(x_inv[...], jnp.concatenate(final, axis=0), 64)
    cells = y_inverse([((lines[:N], c), (lines[N:], c)) for c in range(3)], waves.third, y_inv[...])
    for c in range(3):
        for part in range(2):
            plane = cells[c * N : (c + 1) * N, part * N : (part + 1) * N]
            out[pl.ds(part * 3 + c, N, 6), :] = turn_blocks(plane)


FAST = pltpu.CompilerParams()


def call(kernel, outs, last=False):
    shapes = [jax.ShapeDtypeStruct(s, f32) if last else pltpu.VMEM(s, f32) for s in outs]
    run = pl.pallas_call(kernel, out_shape=shapes if len(shapes) > 1 else shapes[0], name=kernel.__name__, compiler_params=FAST)
    return lambda *args: run(*[pltpu.with_memory_space_constraint(a, pltpu.VMEM) for a in args])


def first_call(v, z_fwd):
    run = pl.pallas_call(
        pencil_to_rows,
        out_shape=pltpu.VMEM((6 * N, N), f32),
        in_specs=[pl.BlockSpec(memory_space=pl.ANY)] * 2,
        scratch_shapes=[pltpu.VMEM(v.shape, f32), pltpu.VMEM(z_fwd.shape, bf16), pltpu.SemaphoreType.DMA((4,))],
        name="pencil_to_rows",
        compiler_params=FAST,
    )
    return run(v, z_fwd)


def exchange(rows):
    count = rows.shape[0] // N
    rows = rows.reshape(N, 1, count * N)
    rows = lax.all_to_all(rows, ("row", "col"), split_axis=0, concat_axis=0, tiled=True)
    return rows.reshape(N * count, N)


TABLES = tables()


def local(velocity):
    t = {name: jnp.asarray(value) for name, value in TABLES.items()}
    kept = (2 * KX, N)

    def physical(rows):
        return call(slab, [(2 * N, N)])(rows, t["mask"], t["z_fwd"], t["z_inv"], t["y_fwd"], t["y_inv"])

    shape = velocity.shape
    rows = exchange(first_call(velocity.reshape(3 * N, N), t["z_fwd"]))
    rows, state = call(start_modes, [(3 * N, N), kept])(rows, t["y_fwd"], t["x_first"], t["x_inv"])
    rows = exchange(physical(exchange(rows)))
    rows, middle, half = call(middle_modes, [(3 * N, N), kept, kept])(rows, t["x_fwd"], t["x_inv"], state)
    rows = exchange(physical(exchange(rows)))
    rows = call(final_modes, [(6 * N, N)])(rows, t["x_fwd"], t["x_inv"], t["y_last"], middle, half)
    return call(rows_to_pencil, [(3 * N, N)], last=True)(exchange(rows), t["z_inv"]).reshape(shape)


def solution(mesh):
    placed = P(None, "row", "col", None)
    return jax.shard_map(local, mesh=mesh, in_specs=(placed,), out_specs=placed, check_vma=False)
```

```python
import jax
import jax.numpy as jnp
import ml_dtypes
import numpy as np
from jax import lax
from jax.experimental import pallas as pl
from jax.experimental.pallas import tpu as pltpu
from jax.sharding import PartitionSpec as P

N = 128
KX = 96
SLOTS = 32
f32, bf16 = jnp.float32, jnp.bfloat16


def owners():
    kz = np.array([1 + d // 3 for d in range(126)] + [0, 0])
    third = np.array([d % 3 for d in range(126)] + [0, 1])
    ky = np.zeros((4, SLOTS), np.int64)
    ok = np.zeros((4, SLOTS), bool)
    ky[0], ok[0] = np.arange(32), True
    ky[1], ok[1] = np.concatenate([np.arange(32, 43), np.arange(-42, -21)]), True
    ky[2, :21], ok[2, :21] = np.arange(-21, 0), True
    return kz, third, ky, ok


def split(a):
    hi = a.astype(np.float32).astype(ml_dtypes.bfloat16)
    lo = (a - hi.astype(np.float64)).astype(np.float32).astype(ml_dtypes.bfloat16)
    return hi, lo


def left(a, pad=0):
    hi, lo = split(a)
    zero = np.zeros((a.shape[0], pad), hi.dtype)
    return np.concatenate([hi, hi, lo, zero], axis=1)


def right(a):
    hi, lo = split(a)
    return np.concatenate([hi, hi, lo], axis=0)


def tables():
    kz, third, ky, ok = owners()
    cell = np.arange(N)

    def angle(a, b):
        return 2 * np.pi * (np.multiply.outer(a, b) % N) / N

    az = angle(kz, cell)
    z_fwd = left(np.concatenate([np.cos(az), -np.sin(az)], axis=0))
    z_inv = left(np.concatenate([np.cos(az.T), -np.sin(az.T)], axis=1))
    ay = angle(ky.reshape(-1), cell)
    keep = ok.reshape(-1)[:, None]
    cy, sy = np.cos(ay) * keep, np.sin(ay) * keep
    y_inv = right(np.block([[cy, sy], [-sy, cy]]))
    y_fwd = right(np.block([[cy.T, -sy.T], [sy.T, cy.T]]))
    ax = angle(np.arange(KX) - 42, cell)
    keep = (np.arange(KX) < 85)[:, None]
    cx, sx = np.cos(ax) * keep, np.sin(ax) * keep
    x_fwd = left(np.block([[cx, sx], [-sx, cx]]))
    x_inv = left(np.block([[cx.T, -sx.T], [sx.T, cx.T]]), 64)
    mask = (np.repeat(np.arange(4), SLOTS)[None, :] == third[:, None]).astype(np.float32)
    flip = np.arange(N) // 8 * 8 + (-np.arange(N)) % 8
    x_first = left(np.block([[cx, sx], [-sx, cx]])[:, np.concatenate([flip, N + flip])])
    back = (np.arange(N) // 16 * -16) % N + np.arange(N) % 16
    y_last = right(np.block([[cy, sy], [-sy, cy]])[:, np.concatenate([back, N + back])])
    return dict(x_first=x_first, y_last=y_last, z_fwd=z_fwd, z_inv=z_inv, y_fwd=y_fwd, y_inv=y_inv, x_fwd=x_fwd, x_inv=x_inv, mask=mask)


def halves(a):
    hi = a.astype(bf16)
    return hi, (a - hi.astype(f32)).astype(bf16)


def dot(a, b):
    return jnp.dot(a, b, preferred_element_type=f32)


def apply_left(table, rows, pad=0):
    hi, lo = halves(rows)
    stack = [hi, lo, hi]
    if pad:
        stack.append(jnp.zeros((pad, rows.shape[1]), bf16))
    return dot(table, jnp.concatenate(stack, axis=0))


def apply_halves(table, rows, pad=0):
    half = table.shape[0] // 2
    return apply_left(table[:half], rows, pad), apply_left(table[half:], rows, pad)


def apply_right(columns, table):
    hi, lo = halves(columns)
    return dot(jnp.concatenate([hi, lo, hi], axis=1), table)


def turn(a, groups):
    shift = (groups * SLOTS) % N
    return pltpu.roll(a, shift, 1) if shift else a


def turn_blocks(a):
    block = (lax.broadcasted_iota(jnp.int32, (N, N), 1) // 16).reshape(16, 8, N)
    a = pltpu.roll(a, 0, 1, stride=16, stride_axis=0).reshape(16, 8, N)
    for bit in (1, 2, 4):
        a = jnp.where((block & bit) == 0, a, pltpu.roll(a, 8 - bit, 1))
    return pltpu.roll(a.reshape(N, N), 0, 1, stride=16, stride_axis=0)


def every(ref, j, count):
    return ref[pl.ds(j, N, count), :]


def pencil_to_rows(v_hbm, z_hbm, out, v, z_fwd, arrived):
    copies = [pltpu.make_async_copy(z_hbm, z_fwd, arrived.at[3])]
    for c in range(3):
        part = pl.ds(c * N, N)
        copies.append(pltpu.make_async_copy(v_hbm.at[part, :], v.at[part, :], arrived.at[c]))
    for copy in copies:
        copy.start()
    for copy in copies:
        copy.wait()
    turned = jnp.concatenate([v[c * N : (c + 1) * N, :].T for c in range(3)], axis=1)
    waves = apply_left(z_fwd[...], turned)
    for part in range(2):
        for c in range(3):
            out[pl.ds(part * 3 + c, N, 6), :] = waves[part * N : (part + 1) * N, c * N : (c + 1) * N]


def rows_to_pencil(rows, z_inv, out_hbm, out, sent):
    copies = []
    stack = jnp.concatenate(
        [jnp.concatenate([every(rows, part * 3 + c, 6) for c in range(3)], axis=1) for part in range(2)], axis=0
    )
    cells = apply_left(z_inv[...], stack)
    for c in range(3):
        part = pl.ds(c * N, N)
        out[part, :] = cells[:, c * N : (c + 1) * N].T
        copies.append(pltpu.make_async_copy(out.at[part, :], out_hbm.at[part, :], sent.at[c]))
        copies[c].start()
    for copy in copies:
        copy.wait()


def y_forward(pairs, mask, table):
    real, imaginary = 0.0, 0.0
    for c in range(3):
        block = apply_right(jnp.concatenate(pairs[c], axis=1), table)
        real = real + turn(block[:, :N] * mask, c)
        imaginary = imaginary + turn(block[:, N:] * mask, c)
    return real, imaginary


def y_inverse(places, mask, table):
    stack = [jnp.concatenate([turn(a, -group) * mask for a, group in pair], axis=1) for pair in places]
    parts = [jnp.concatenate(stack[i : i + 3], axis=0) for i in range(0, len(stack), 3)]
    return jnp.concatenate([apply_right(p, table) for p in parts], axis=0)


def slab(rows, mask, z_fwd, z_inv, y_fwd, y_inv, out):
    mask = mask[...]
    real, imaginary, rest = (every(rows, j, 3) for j in range(3))
    places = [((real, f), (imaginary, f)) for f in range(4)] + [((rest, f), (rest, f + 2)) for f in (1, 2)]
    lines = y_inverse(places, mask, y_inv[...])
    fields = [lines[f * N : (f + 1) * N] for f in range(6)]
    stack = jnp.concatenate(
        [jnp.concatenate([a[:, part * N : (part + 1) * N] for a in fields], axis=1) for part in range(2)], axis=0
    )
    grid = apply_left(z_inv[...], stack)
    u = [grid[:, c * N : (c + 1) * N] for c in range(3)]
    w = [grid[:, (3 + c) * N : (4 + c) * N] for c in range(3)]
    product = jnp.concatenate(
        [u[1] * w[2] - u[2] * w[1], u[2] * w[0] - u[0] * w[2], u[0] * w[1] - u[1] * w[0]], axis=1
    )
    waves = apply_left(z_fwd[...], product)
    pairs = [(waves[:N, c * N : (c + 1) * N], waves[N:, c * N : (c + 1) * N]) for c in range(3)]
    real, imaginary = y_forward(pairs, mask, y_fwd[...])
    out[pl.ds(0, N, 2), :] = real
    out[pl.ds(1, N, 2), :] = imaginary


class Waves:
    def __init__(self):
        device = lax.axis_index("row") * lax.axis_size("col") + lax.axis_index("col")
        kz = jnp.where(device < 126, 1 + lax.div(device, 3), 0)
        third = jnp.where(device < 126, lax.rem(device, 3), device - 126)
        lane = lax.broadcasted_iota(jnp.int32, (1, N), 1)
        group, slot = lane // SLOTS, lane % SLOTS
        c = (group - third + 4) % 4
        wrapped = jnp.where(slot < 11, slot + 32, slot - 53)
        ky = jnp.where(third == 0, slot, jnp.where(third == 1, wrapped, slot - 21))
        good = (c < 3) & ((third < 2) | (slot < 21)) & ((kz > 0) | (ky >= 0))
        count = jnp.where((kz == 0) & (ky == 0), 1.0, 2.0)
        kx = lax.broadcasted_iota(jnp.int32, (KX, N), 0) - 42

        def component(x, y, z):
            return jnp.where(c == x, kx, jnp.where(c == y, ky, jnp.where(c == z, kz, 0))).astype(f32)

        self.own = component(0, 1, 2)
        self.after = component(2, 0, 1)
        self.before = component(1, 2, 0)
        self.squared = (kx * kx + (ky * ky + kz * kz)).astype(f32)
        self.inverse = 1.0 / jnp.where(self.squared > 0, self.squared, 1.0)
        self.scale = jnp.where(good, count * (1.0 / N**3), 0.0)
        whole = jnp.broadcast_to(c, (KX, N))
        self.is_last = whole == 2
        self.is_first = whole == 0
        self.is_free = whole == 3
        lines = jnp.broadcast_to(c, (N, N))
        self.has_rest = (lines == 1) | (lines == 2)
        self.third = (group == third).astype(f32)

    def project(self, part):
        part = part * self.scale
        along = part * self.own
        along = along + turn(along, 1)
        along = along + turn(along, 2)
        return part - self.own * (along * self.inverse)

    def cross(self, part):
        two = turn(part, 2)
        after = jnp.where(self.is_last, two, turn(part, -1))
        before = jnp.where(self.is_first, two, turn(part, 1))
        return self.after * before - self.before * after


def x_forward(real, imaginary, table):
    waves = apply_left(table, jnp.concatenate([real, imaginary], axis=0))
    return waves[:KX], waves[KX:]


def send_fields(waves, state, x_inv, out):
    curl = (-waves.cross(state[1]), waves.cross(state[0]))
    both = [jnp.where(waves.is_free, turn(curl[i], 3), state[i]) for i in range(2)]
    stack = jnp.concatenate([jnp.concatenate([both[i], curl[i]], axis=1) for i in range(2)], axis=0)
    lines = apply_halves(x_inv[...], stack, 64)
    for part in range(2):
        out[pl.ds(part, N, 3), :] = lines[part][:, :N]
    out[pl.ds(2, N, 3), :] = jnp.where(waves.has_rest, lines[0][:, N:], turn(lines[1][:, N:], 2))


def start_modes(rows, y_fwd, x_fwd, x_inv, out, state_out):
    waves = Waves()
    planes = [turn_blocks(every(rows, j, 6)) for j in range(6)]
    real, imaginary = y_forward([(planes[c], planes[3 + c]) for c in range(3)], waves.third, y_fwd[...])
    state = [waves.project(part) for part in x_forward(real, imaginary, x_fwd[...])]
    for i in range(2):
        state_out[i * KX : (i + 1) * KX, :] = state[i]
    send_fields(waves, state, x_inv, out)


def tendency(waves, rows, x_fwd, state):
    parts = x_forward(every(rows, 0, 2), every(rows, 1, 2), x_fwd[...])
    viscous = waves.squared * (1.0 / N)
    return [waves.project(parts[i]) - viscous * state[i] for i in range(2)]


def middle_modes(rows, x_fwd, x_inv, state_in, out, middle_out, half_out):
    waves = Waves()
    state = [state_in[i * KX : (i + 1) * KX, :] for i in range(2)]
    first = tendency(waves, rows, x_fwd, state)
    step = 2.0 / N
    middle = [state[i] + step * first[i] for i in range(2)]
    for i in range(2):
        middle_out[i * KX : (i + 1) * KX, :] = middle[i]
        half_out[i * KX : (i + 1) * KX, :] = state[i] + 0.5 * step * first[i]
    send_fields(waves, middle, x_inv, out)


def final_modes(rows, x_fwd, x_inv, y_inv, middle_in, half_in, out):
    waves = Waves()
    middle = [middle_in[i * KX : (i + 1) * KX, :] for i in range(2)]
    second = tendency(waves, rows, x_fwd, middle)
    final = [half_in[i * KX : (i + 1) * KX, :] + (1.0 / N) * second[i] for i in range(2)]
    lines = apply_left(x_inv[...], jnp.concatenate(final, axis=0), 64)
    cells = y_inverse([((lines[:N], c), (lines[N:], c)) for c in range(3)], waves.third, y_inv[...])
    for c in range(3):
        for part in range(2):
            plane = cells[c * N : (c + 1) * N, part * N : (part + 1) * N]
            out[pl.ds(part * 3 + c, N, 6), :] = turn_blocks(plane)


FAST = pltpu.CompilerParams()


def call(kernel, outs):
    shapes = [pltpu.VMEM(s, f32) for s in outs]
    run = pl.pallas_call(kernel, out_shape=shapes if len(shapes) > 1 else shapes[0], name=kernel.__name__, compiler_params=FAST)
    return lambda *args: run(*[pltpu.with_memory_space_constraint(a, pltpu.VMEM) for a in args])


def first_call(v, z_fwd):
    run = pl.pallas_call(
        pencil_to_rows,
        out_shape=pltpu.VMEM((6 * N, N), f32),
        in_specs=[pl.BlockSpec(memory_space=pl.ANY)] * 2,
        scratch_shapes=[pltpu.VMEM(v.shape, f32), pltpu.VMEM(z_fwd.shape, bf16), pltpu.SemaphoreType.DMA((4,))],
        name="pencil_to_rows",
        compiler_params=FAST,
    )
    return run(v, z_fwd)


def last_call(rows, z_inv):
    shape = (3 * N, N)
    run = pl.pallas_call(
        rows_to_pencil,
        out_shape=jax.ShapeDtypeStruct(shape, f32),
        out_specs=pl.BlockSpec(memory_space=pl.ANY),
        scratch_shapes=[pltpu.VMEM(shape, f32), pltpu.SemaphoreType.DMA((3,))],
        name="rows_to_pencil",
        compiler_params=FAST,
    )
    return run(*[pltpu.with_memory_space_constraint(a, pltpu.VMEM) for a in (rows, z_inv)])


def exchange(rows):
    count = rows.shape[0] // N
    rows = rows.reshape(N, 1, count * N)
    rows = lax.all_to_all(rows, ("row", "col"), split_axis=0, concat_axis=0, tiled=True)
    return rows.reshape(N * count, N)


TABLES = tables()


def local(velocity):
    t = {name: jnp.asarray(value) for name, value in TABLES.items()}
    kept = (2 * KX, N)

    def physical(rows):
        return call(slab, [(2 * N, N)])(rows, t["mask"], t["z_fwd"], t["z_inv"], t["y_fwd"], t["y_inv"])

    shape = velocity.shape
    rows = exchange(first_call(velocity.reshape(3 * N, N), t["z_fwd"]))
    rows, state = call(start_modes, [(3 * N, N), kept])(rows, t["y_fwd"], t["x_first"], t["x_inv"])
    rows = exchange(physical(exchange(rows)))
    rows, middle, half = call(middle_modes, [(3 * N, N), kept, kept])(rows, t["x_fwd"], t["x_inv"], state)
    rows = exchange(physical(exchange(rows)))
    rows = call(final_modes, [(6 * N, N)])(rows, t["x_fwd"], t["x_inv"], t["y_last"], middle, half)
    return last_call(exchange(rows), t["z_inv"]).reshape(shape)


def solution(mesh):
    placed = P(None, "row", "col", None)
    return jax.shard_map(local, mesh=mesh, in_specs=(placed,), out_specs=placed, check_vma=False)
```

```python
import jax
import jax.numpy as jnp
import ml_dtypes
import numpy as np
from jax import lax
from jax.experimental import pallas as pl
from jax.experimental.pallas import tpu as pltpu
from jax.sharding import PartitionSpec as P

N = 128
KX = 96
SLOTS = 32
f32, bf16 = jnp.float32, jnp.bfloat16


def owners():
    kz = np.array([1 + d // 3 for d in range(126)] + [0, 0])
    third = np.array([d % 3 for d in range(126)] + [0, 1])
    ky = np.zeros((4, SLOTS), np.int64)
    ok = np.zeros((4, SLOTS), bool)
    ky[0], ok[0] = np.arange(32), True
    ky[1], ok[1] = np.concatenate([np.arange(32, 43), np.arange(-42, -21)]), True
    ky[2, :21], ok[2, :21] = np.arange(-21, 0), True
    return kz, third, ky, ok


def split(a):
    hi = a.astype(np.float32).astype(ml_dtypes.bfloat16)
    lo = (a - hi.astype(np.float64)).astype(np.float32).astype(ml_dtypes.bfloat16)
    return hi, lo


def left(a, pad=0):
    hi, lo = split(a)
    zero = np.zeros((a.shape[0], pad), hi.dtype)
    return np.concatenate([hi, hi, lo, zero], axis=1)


def right(a):
    return np.concatenate(split(a), axis=0)


def tables():
    kz, third, ky, ok = owners()
    cell = np.arange(N)

    def angle(a, b):
        return 2 * np.pi * (np.multiply.outer(a, b) % N) / N

    az = angle(kz, cell)
    z_fwd = left(np.concatenate([np.cos(az), -np.sin(az)], axis=0))
    z_inv = left(np.concatenate([np.cos(az.T), -np.sin(az.T)], axis=1))
    ay = angle(ky.reshape(-1), cell)
    keep = ok.reshape(-1)[:, None]
    cy, sy = np.cos(ay) * keep, np.sin(ay) * keep
    y_inv = right(np.block([[cy, sy], [-sy, cy]]))
    shifts = [[np.roll(a, SLOTS * c, axis=1) for a in (cy.T, sy.T)] for c in range(3)]
    y_fwd = np.concatenate([right(np.block([[a, -b], [b, a]])) for a, b in shifts], axis=0)
    ax = angle(np.arange(KX) - 42, cell)
    keep = (np.arange(KX) < 85)[:, None]
    cx, sx = np.cos(ax) * keep, np.sin(ax) * keep
    x_fwd = left(np.block([[cx, sx], [-sx, cx]]))
    x_inv = left(np.block([[cx.T, -sx.T], [sx.T, cx.T]]), 64)
    held = ((np.repeat(np.arange(4), SLOTS)[None, :] - third[:, None]) % 4).astype(np.int32)
    flip = np.arange(N) // 8 * 8 + (-np.arange(N)) % 8
    x_first = left(np.block([[cx, sx], [-sx, cx]])[:, np.concatenate([flip, N + flip])])
    back = (np.arange(N) // 16 * -16) % N + np.arange(N) % 16
    y_last = right(np.block([[cy, sy], [-sy, cy]])[:, np.concatenate([back, N + back])])
    return dict(x_first=x_first, y_last=y_last, z_fwd=z_fwd, z_inv=z_inv, y_fwd=y_fwd, y_inv=y_inv, x_fwd=x_fwd, x_inv=x_inv, held=held)


def halves(a):
    hi = a.astype(bf16)
    return hi, (a - hi.astype(f32)).astype(bf16)


def dot(a, b):
    return jnp.dot(a, b, preferred_element_type=f32)


def apply_left(table, rows, pad=0):
    hi, lo = halves(rows)
    stack = [hi, lo, hi]
    if pad:
        stack.append(jnp.zeros((pad, rows.shape[1]), bf16))
    return dot(table, jnp.concatenate(stack, axis=0))


def apply_halves(table, rows, pad=0):
    half = table.shape[0] // 2
    return apply_left(table[:half], rows, pad), apply_left(table[half:], rows, pad)


def apply_right(columns, table):
    hi, lo = halves(columns)
    return dot(jnp.concatenate([hi, lo, hi], axis=1), jnp.concatenate([table[: 2 * N], table], axis=0))


def turn(a, groups):
    shift = (groups * SLOTS) % N
    return pltpu.roll(a, shift, 1) if shift else a


def turn_blocks(a):
    block = (lax.broadcasted_iota(jnp.int32, (N, N), 1) // 16).reshape(16, 8, N)
    a = pltpu.roll(a, 0, 1, stride=16, stride_axis=0).reshape(16, 8, N)
    for bit in (1, 2, 4):
        a = jnp.where((block & bit) == 0, a, pltpu.roll(a, 8 - bit, 1))
    return pltpu.roll(a.reshape(N, N), 0, 1, stride=16, stride_axis=0)


def every(ref, j, count):
    return ref[pl.ds(j, N, count), :]


def pencil_to_rows(v_hbm, z_hbm, out, v, z_fwd, arrived):
    copies = [pltpu.make_async_copy(z_hbm, z_fwd, arrived.at[3])]
    for c in range(3):
        part = pl.ds(c * N, N)
        copies.append(pltpu.make_async_copy(v_hbm.at[part, :], v.at[part, :], arrived.at[c]))
    for copy in copies:
        copy.start()
    for copy in copies:
        copy.wait()
    turned = jnp.concatenate([v[c * N : (c + 1) * N, :].T for c in range(3)], axis=1)
    waves = apply_left(z_fwd[...], turned)
    for part in range(2):
        for c in range(3):
            out[pl.ds(part * 3 + c, N, 6), :] = waves[part * N : (part + 1) * N, c * N : (c + 1) * N]


def rows_to_pencil(rows, z_inv, out_hbm, out, sent):
    copies = []
    stack = jnp.concatenate(
        [jnp.concatenate([every(rows, part * 3 + c, 6) for c in range(3)], axis=1) for part in range(2)], axis=0
    )
    cells = apply_left(z_inv[...], stack)
    for c in range(3):
        part = pl.ds(c * N, N)
        out[part, :] = cells[:, c * N : (c + 1) * N].T
        copies.append(pltpu.make_async_copy(out.at[part, :], out_hbm.at[part, :], sent.at[c]))
        copies[c].start()
    for copy in copies:
        copy.wait()


def y_forward(pairs, held, table):
    real, imaginary = 0.0, 0.0
    for c in range(3):
        block = apply_right(jnp.concatenate(pairs[c], axis=1), table[4 * N * c : 4 * N * (c + 1), :])
        real = jnp.where(held == c, block[:, :N], real)
        imaginary = jnp.where(held == c, block[:, N:], imaginary)
    return real, imaginary


def y_inverse(places, held, table):
    lines = []
    for pair in places:
        columns = jnp.concatenate([jnp.where(held == group % 4, a, 0.0) for a, group in pair], axis=1)
        rows = []
        for half in range(2):
            for part in range(2):
                for g in range(4):
                    start = (2 * half + part) * N + (g - pair[part][1]) % 4 * SLOTS
                    rows.append(table[start : start + SLOTS, :])
        lines.append(apply_right(columns, jnp.concatenate(rows, axis=0)))
    return jnp.concatenate(lines, axis=0)


def slab(rows, held, z_fwd, z_inv, y_fwd, y_inv, out):
    held = held[...]
    real, imaginary, rest = (every(rows, j, 3) for j in range(3))
    places = [((real, f), (imaginary, f)) for f in range(4)] + [((rest, f), (rest, f + 2)) for f in (1, 2)]
    lines = y_inverse(places, held, y_inv)
    fields = [lines[f * N : (f + 1) * N] for f in range(6)]
    stack = jnp.concatenate(
        [jnp.concatenate([a[:, part * N : (part + 1) * N] for a in fields], axis=1) for part in range(2)], axis=0
    )
    grid = apply_left(z_inv[...], stack)
    u = [grid[:, c * N : (c + 1) * N] for c in range(3)]
    w = [grid[:, (3 + c) * N : (4 + c) * N] for c in range(3)]
    product = jnp.concatenate(
        [u[1] * w[2] - u[2] * w[1], u[2] * w[0] - u[0] * w[2], u[0] * w[1] - u[1] * w[0]], axis=1
    )
    waves = apply_left(z_fwd[...], product)
    pairs = [(waves[:N, c * N : (c + 1) * N], waves[N:, c * N : (c + 1) * N]) for c in range(3)]
    real, imaginary = y_forward(pairs, held, y_fwd)
    out[pl.ds(0, N, 2), :] = real
    out[pl.ds(1, N, 2), :] = imaginary


class Waves:
    def __init__(self):
        device = lax.axis_index("row") * lax.axis_size("col") + lax.axis_index("col")
        kz = jnp.where(device < 126, 1 + lax.div(device, 3), 0)
        third = jnp.where(device < 126, lax.rem(device, 3), device - 126)
        lane = lax.broadcasted_iota(jnp.int32, (1, N), 1)
        group, slot = lane // SLOTS, lane % SLOTS
        c = (group - third + 4) % 4
        wrapped = jnp.where(slot < 11, slot + 32, slot - 53)
        ky = jnp.where(third == 0, slot, jnp.where(third == 1, wrapped, slot - 21))
        good = (c < 3) & ((third < 2) | (slot < 21)) & ((kz > 0) | (ky >= 0))
        count = jnp.where((kz == 0) & (ky == 0), 1.0, 2.0)
        kx = lax.broadcasted_iota(jnp.int32, (KX, N), 0) - 42

        def component(x, y, z):
            return jnp.where(c == x, kx, jnp.where(c == y, ky, jnp.where(c == z, kz, 0))).astype(f32)

        self.own = component(0, 1, 2)
        self.after = component(2, 0, 1)
        self.before = component(1, 2, 0)
        self.squared = (kx * kx + (ky * ky + kz * kz)).astype(f32)
        self.inverse = 1.0 / jnp.where(self.squared > 0, self.squared, 1.0)
        self.scale = jnp.where(good, count * (1.0 / N**3), 0.0)
        whole = jnp.broadcast_to(c, (KX, N))
        self.is_last = whole == 2
        self.is_first = whole == 0
        self.is_free = whole == 3
        self.held = jnp.broadcast_to(c, (N, N))
        self.has_rest = (self.held == 1) | (self.held == 2)

    def project(self, part):
        part = part * self.scale
        along = part * self.own
        along = along + turn(along, 1)
        along = along + turn(along, 2)
        return part - self.own * (along * self.inverse)

    def cross(self, part):
        two = turn(part, 2)
        after = jnp.where(self.is_last, two, turn(part, -1))
        before = jnp.where(self.is_first, two, turn(part, 1))
        return self.after * before - self.before * after


def x_forward(real, imaginary, table):
    waves = apply_left(table, jnp.concatenate([real, imaginary], axis=0))
    return waves[:KX], waves[KX:]


def send_fields(waves, state, x_inv, out):
    curl = (-waves.cross(state[1]), waves.cross(state[0]))
    both = [jnp.where(waves.is_free, turn(curl[i], 3), state[i]) for i in range(2)]
    stack = jnp.concatenate([jnp.concatenate([both[i], curl[i]], axis=1) for i in range(2)], axis=0)
    lines = apply_halves(x_inv[...], stack, 64)
    for part in range(2):
        out[pl.ds(part, N, 3), :] = lines[part][:, :N]
    out[pl.ds(2, N, 3), :] = jnp.where(waves.has_rest, lines[0][:, N:], turn(lines[1][:, N:], 2))


def start_modes(rows, y_fwd, x_fwd, x_inv, out, state_out):
    waves = Waves()
    planes = [turn_blocks(every(rows, j, 6)) for j in range(6)]
    real, imaginary = y_forward([(planes[c], planes[3 + c]) for c in range(3)], waves.held, y_fwd)
    state = [waves.project(part) for part in x_forward(real, imaginary, x_fwd[...])]
    for i in range(2):
        state_out[i * KX : (i + 1) * KX, :] = state[i]
    send_fields(waves, state, x_inv, out)


def tendency(waves, rows, x_fwd, state):
    parts = x_forward(every(rows, 0, 2), every(rows, 1, 2), x_fwd[...])
    viscous = waves.squared * (1.0 / N)
    return [waves.project(parts[i]) - viscous * state[i] for i in range(2)]


def middle_modes(rows, x_fwd, x_inv, state_in, out, middle_out, half_out):
    waves = Waves()
    state = [state_in[i * KX : (i + 1) * KX, :] for i in range(2)]
    first = tendency(waves, rows, x_fwd, state)
    step = 2.0 / N
    middle = [state[i] + step * first[i] for i in range(2)]
    for i in range(2):
        middle_out[i * KX : (i + 1) * KX, :] = middle[i]
        half_out[i * KX : (i + 1) * KX, :] = state[i] + 0.5 * step * first[i]
    send_fields(waves, middle, x_inv, out)


def final_modes(rows, x_fwd, x_inv, y_inv, middle_in, half_in, out):
    waves = Waves()
    middle = [middle_in[i * KX : (i + 1) * KX, :] for i in range(2)]
    second = tendency(waves, rows, x_fwd, middle)
    final = [half_in[i * KX : (i + 1) * KX, :] + (1.0 / N) * second[i] for i in range(2)]
    lines = apply_left(x_inv[...], jnp.concatenate(final, axis=0), 64)
    cells = y_inverse([((lines[:N], c), (lines[N:], c)) for c in range(3)], waves.held, y_inv)
    for c in range(3):
        for part in range(2):
            plane = cells[c * N : (c + 1) * N, part * N : (part + 1) * N]
            out[pl.ds(part * 3 + c, N, 6), :] = turn_blocks(plane)


FAST = pltpu.CompilerParams()


def call(kernel, outs):
    shapes = [pltpu.VMEM(s, f32) for s in outs]
    run = pl.pallas_call(kernel, out_shape=shapes if len(shapes) > 1 else shapes[0], name=kernel.__name__, compiler_params=FAST)
    return lambda *args: run(*[pltpu.with_memory_space_constraint(a, pltpu.VMEM) for a in args])


def first_call(v, z_fwd):
    run = pl.pallas_call(
        pencil_to_rows,
        out_shape=pltpu.VMEM((6 * N, N), f32),
        in_specs=[pl.BlockSpec(memory_space=pl.ANY)] * 2,
        scratch_shapes=[pltpu.VMEM(v.shape, f32), pltpu.VMEM(z_fwd.shape, bf16), pltpu.SemaphoreType.DMA((4,))],
        name="pencil_to_rows",
        compiler_params=FAST,
    )
    return run(v, z_fwd)


def last_call(rows, z_inv):
    shape = (3 * N, N)
    run = pl.pallas_call(
        rows_to_pencil,
        out_shape=jax.ShapeDtypeStruct(shape, f32),
        out_specs=pl.BlockSpec(memory_space=pl.ANY),
        scratch_shapes=[pltpu.VMEM(shape, f32), pltpu.SemaphoreType.DMA((3,))],
        name="rows_to_pencil",
        compiler_params=FAST,
    )
    return run(*[pltpu.with_memory_space_constraint(a, pltpu.VMEM) for a in (rows, z_inv)])


def exchange(rows):
    count = rows.shape[0] // N
    rows = rows.reshape(N, 1, count * N)
    rows = lax.all_to_all(rows, ("row", "col"), split_axis=0, concat_axis=0, tiled=True)
    return rows.reshape(N * count, N)


TABLES = tables()


def local(velocity):
    t = {name: jnp.asarray(value) for name, value in TABLES.items()}
    kept = (2 * KX, N)

    def physical(rows):
        return call(slab, [(2 * N, N)])(rows, t["held"], t["z_fwd"], t["z_inv"], t["y_fwd"], t["y_inv"])

    shape = velocity.shape
    rows = exchange(first_call(velocity.reshape(3 * N, N), t["z_fwd"]))
    rows, state = call(start_modes, [(3 * N, N), kept])(rows, t["y_fwd"], t["x_first"], t["x_inv"])
    rows = exchange(physical(exchange(rows)))
    rows, middle, half = call(middle_modes, [(3 * N, N), kept, kept])(rows, t["x_fwd"], t["x_inv"], state)
    rows = exchange(physical(exchange(rows)))
    rows = call(final_modes, [(6 * N, N)])(rows, t["x_fwd"], t["x_inv"], t["y_last"], middle, half)
    return last_call(exchange(rows), t["z_inv"]).reshape(shape)


def solution(mesh):
    placed = P(None, "row", "col", None)
    return jax.shard_map(local, mesh=mesh, in_specs=(placed,), out_specs=placed, check_vma=False)
```
